128 devices in a mesh: sp: 8 (over z, core), tp: 16 (over x, y).
Axes of the slice: x: 4, y: 4, z: 4, core: 2. Of those that a mesh axis runs over, the one named last changes fastest.
Arguments:
- tokens: bfloat16 [16384, 2048], P(('sp', 'tp')), may hold values from -3 to 3
- queries: bfloat16 [16384, 2048], P(('sp', 'tp')), may hold values from -140 to 140
- keys: bfloat16 [16384, 1024], P(('sp', 'tp')), may hold values from -6 to 6
- values: bfloat16 [16384, 1024], P(('sp', 'tp')), may hold values from -6 to 6
- out_weight: bfloat16 [2048, 2048], P('sp', 'tp'), may hold values from -0.25 to 0.25
- norm_gain: bfloat16 [2048], replicated, may hold values from 0.099609375 to 1.8984375
- gate_weight: bfloat16 [2048, 7168], P('sp', 'tp'), may hold values from -0.125 to 0.125
- up_weight: bfloat16 [2048, 7168], P('sp', 'tp'), may hold values from -0.125 to 0.125
- down_weight: bfloat16 [7168, 2048], P('tp', 'sp'), may hold values from -0.125 to 0.125
Outputs:
- attended: bfloat16 [16384, 2048], P(('sp', 'tp'))
- layer_out: bfloat16 [16384, 2048], P(('sp', 'tp'))
The draws below stay inside these ranges and needn't reach their ends.
All inputs are finite; a program needn't handle non-finite values.
Results may differ from the reference program's by a relative error of at most 0.023.
Values may be sent and summed in bfloat16 or wider, within the bound.
No kernel may reach another device: no remote copies, remote signals or barrier semaphores. Data moves between devices by JAX's collectives and lax.ppermute only.
A program may use at most 128 MiB of HBM per device.

```python
import jax
import jax.numpy as jnp
from jax import lax

D = 2048
FF = 7168
HEADS = 16
KV_HEADS = 8
HEAD_DIM = 128
TOK_DEV = 2048
SEQ = 16384
N_TP = 16


def shared_keys(key):
    sub_key = jax.random.fold_in(key, 5)
    base_draw = jnp.clip(jax.random.normal(sub_key, (SEQ, KV_HEADS * HEAD_DIM), jnp.float32), -5.0, 5.0)
    return base_draw


def draw_keys(key, part):
    return shared_keys(key).astype(jnp.bfloat16)


def draw_queries(key, part):
    sub_key = jax.random.fold_in(key, 9)
    base_draw = jnp.clip(2.5 * jax.random.normal(sub_key, (SEQ, HEADS * HEAD_DIM), jnp.float32), -15.0, 15.0)
    return base_draw.astype(jnp.bfloat16)


def level_of(own_key, dims, cuts, smallest, high):
    level = 1.0
    for position, shards_of in cuts:
        steps = jax.random.uniform(jax.random.fold_in(jax.random.fold_in(own_key, 6), position), (shards_of,), jnp.float32, smallest / len(cuts), high / len(cuts))
        level = level * jnp.repeat(jnp.exp(steps), dims[position] // shards_of).reshape((-1,) + (1,) * (len(dims) - 1 - position))
    return level


def scatter_about(stream_key, dims, width, most, shards=(), held_as=jnp.bfloat16):
    result = width * jax.random.normal(stream_key, dims, jnp.float32)
    if shards:
        result = result * level_of(stream_key, dims, shards, -0.22, 0.18)
    return jnp.clip(result, -most, most).astype(held_as)


def setup_inputs(seed: int = 0) -> dict:
    splits = jax.random.split(jax.random.key(seed), 10)
    return {
        "tokens": scatter_about(splits[0], (SEQ, D), 0.5, 3.0, ((0, 128),)),
        "queries": draw_queries(jax.random.fold_in(splits[9], 71), 0),
        "keys": draw_keys(jax.random.fold_in(splits[9], 71), 0),
        "values": scatter_about(splits[3], (SEQ, KV_HEADS * HEAD_DIM), 1.0, 6.0, ((0, 128),)),
        "out_weight": scatter_about(splits[4], (HEADS * HEAD_DIM, D), (HEADS * HEAD_DIM // 4) ** -0.5, 0.25, ((0, 8), (1, 16))),
        "norm_gain": jnp.clip(1.0 + 0.18 * jax.random.normal(splits[5], (D,), jnp.float32), 0.099609375, 1.8984375).astype(jnp.bfloat16),
        "gate_weight": scatter_about(splits[6], (D, FF), D ** -0.5, 0.125, ((0, 8), (1, 16))),
        "up_weight": scatter_about(splits[7], (D, FF), D ** -0.5, 0.125, ((0, 8), (1, 16))),
        "down_weight": scatter_about(splits[8], (FF, D), (FF // 4) ** -0.5, 0.125, ((0, 16), (1, 8))),
    }


def one_group(inputs):
    q_head, k_head, v_head = inputs
    seq_len = k_head.shape[0]
    group_size = q_head.shape[1]
    k_wide = k_head.astype(jnp.float32)
    v_wide = v_head.astype(jnp.float32)
    block_count = seq_len // TOK_DEV
    q_blocks = q_head.reshape(block_count, TOK_DEV, group_size, HEAD_DIM)
    starts = jnp.arange(block_count, dtype=jnp.int32) * TOK_DEV
    key_pos = jnp.arange(seq_len, dtype=jnp.int32)

    def one_block(pair):
        q_block, start = pair
        scores = jnp.einsum('qgd,kd->gqk', q_block.astype(jnp.float32), k_wide) * HEAD_DIM ** (-0.5)
        query_pos = start + jnp.arange(TOK_DEV, dtype=jnp.int32)
        causal = key_pos[None, :] <= query_pos[:, None]
        scores = jnp.where(causal[None, :, :], scores, -1e+30)
        row_peak = lax.optimization_barrier(jnp.max(scores, axis=-1, keepdims=True))
        exp_terms = jnp.exp(scores - row_peak)
        probs = (exp_terms / lax.optimization_barrier(jnp.sum(exp_terms, axis=-1, keepdims=True))).astype(jnp.bfloat16)
        mixed_out = jnp.einsum('gqk,kd->qgd', probs.astype(jnp.float32), v_wide)
        return mixed_out.astype(jnp.bfloat16)
    blocks_out = lax.map(one_block, (q_blocks, starts))
    return blocks_out.reshape(seq_len, group_size, HEAD_DIM)

def reference(tokens, queries, keys, values, out_weight, norm_gain, gate_weight, up_weight, down_weight):
    seq_len = tokens.shape[0]
    group_size = HEADS // KV_HEADS
    q_stack = jnp.transpose(queries.reshape(seq_len, KV_HEADS, group_size, HEAD_DIM), (1, 0, 2, 3))
    k_stack = jnp.transpose(keys.reshape(seq_len, KV_HEADS, HEAD_DIM), (1, 0, 2))
    v_stack = jnp.transpose(values.reshape(seq_len, KV_HEADS, HEAD_DIM), (1, 0, 2))
    grouped = lax.map(one_group, (q_stack, k_stack, v_stack))
    attn = jnp.transpose(grouped, (1, 0, 2, 3)).reshape(seq_len, HEADS * HEAD_DIM)
    projected = jnp.dot(attn, out_weight, preferred_element_type=jnp.float32)
    attended = (tokens.astype(jnp.float32) + projected).astype(jnp.bfloat16)
    attended_wide = attended.astype(jnp.float32)
    inverse_rms = lax.rsqrt(lax.optimization_barrier(jnp.mean(attended_wide * attended_wide, axis=1, keepdims=True)) + 1e-05)
    normed = (attended_wide * inverse_rms * norm_gain.astype(jnp.float32)).astype(jnp.bfloat16)
    gate_sum = jnp.dot(normed, gate_weight, preferred_element_type=jnp.float32)
    up_sum = jnp.dot(normed, up_weight, preferred_element_type=jnp.float32)
    hidden = (jax.nn.silu(gate_sum) * up_sum).astype(jnp.bfloat16)
    block_width = FF // N_TP
    hidden_blocks = jnp.transpose(hidden.reshape(seq_len, N_TP, block_width), (1, 0, 2))
    down_blocks = down_weight.reshape(N_TP, block_width, D)

    def add_block(total, pair):
        hidden_block, down_block = pair
        partial_value = jnp.dot(hidden_block, down_block, preferred_element_type=jnp.float32).astype(jnp.bfloat16)
        partial_value = lax.optimization_barrier(partial_value)
        return (total + partial_value.astype(jnp.float32), None)
    ffn_part, _ = lax.scan(add_block, jnp.zeros((seq_len, D), jnp.float32), (hidden_blocks, down_blocks))
    layer_out = (attended_wide + ffn_part).astype(jnp.bfloat16)
    return (attended, layer_out)
```

```python
import functools

import jax
import jax.numpy as jnp
import numpy as np
from jax import lax
from jax.experimental import pallas as pl
from jax.experimental.pallas import tpu as pltpu
from jax.sharding import Mesh
from jax.sharding import PartitionSpec as P

HEAD_DIM = 128
EPS = 1e-05
ROWS = 128
Z, C, X, Y = 4, 2, 4, 4
HEADS = Z * X
BLOCK = X * ROWS
LOCAL = Z * BLOCK
SCALE = float(HEAD_DIM**-0.5 * np.log2(np.e))
VMEM = 58 * 1024 * 1024
F32 = jnp.float32
BF16 = jnp.bfloat16


def params():
    return pltpu.CompilerParams(vmem_limit_bytes=VMEM)


def along_y(array, step):
    return lax.ppermute(array, "y", [(i, (i + step) % Y) for i in range(Y)])


def other_core(array):
    return lax.ppermute(array, "c", [(0, 1), (1, 0)])


def attend_body(first, last, n_pairs, where_ref, q_ref, *refs):
    kv_refs = refs[: 2 * n_pairs]
    refs = refs[2 * n_pairs :]
    if first:
        m_in = l_in = a_in = None
    else:
        m_in, l_in, a_in = refs[:3]
        refs = refs[3:]
    if last:
        (o_ref,) = refs[:1]
        kv_s, m_s, l_s, a_s = refs[1:]
    else:
        m_s, l_s, a_s = refs[:3]
        (kv_s,) = refs[3:]
    for i in range(2 * n_pairs):
        kv_s[i] = kv_refs[i][...]
    c_q = where_ref[0]
    y_q = where_ref[1]

    def scores(q, pair, zk, core):
        k = kv_s[2 * pair + core, pl.ds(zk * BLOCK, BLOCK), :HEAD_DIM]
        return lax.dot_general(q, k, (((1,), (1,)), ((), ())), preferred_element_type=F32) * SCALE

    def accumulate(rows, s_two, pair, zk):
        m_old = m_s[rows, :]
        peak = jnp.maximum(
            jnp.max(s_two[0], axis=1, keepdims=True), jnp.max(s_two[1], axis=1, keepdims=True)
        )
        m_new = jnp.maximum(m_old, jnp.broadcast_to(peak, m_old.shape))
        alpha = jnp.exp2(m_old - m_new)
        l_new = l_s[rows, :] * alpha
        a_new = a_s[rows, :] * alpha
        for core in range(2):
            p = jnp.exp2(s_two[core] - m_new[:, :1])
            for lane in range(BLOCK // 128):
                l_new = l_new + p[:, lane * 128 : (lane + 1) * 128]
            v = kv_s[2 * pair + core, pl.ds(zk * BLOCK, BLOCK), HEAD_DIM:]
            a_new = a_new + lax.dot_general(
                p.astype(BF16), v, (((1,), (0,)), ((), ())), preferred_element_type=F32
            )
        m_s[rows, :] = m_new
        l_s[rows, :] = l_new
        a_s[rows, :] = a_new

    q_row = lax.broadcasted_iota(jnp.int32, (BLOCK, BLOCK), 0)
    k_row = lax.broadcasted_iota(jnp.int32, (BLOCK, BLOCK), 1)
    ahead = (k_row // ROWS - q_row // ROWS) * (Y * ROWS) + (k_row % ROWS - q_row % ROWS)

    def per_z(zq, _):
        rows = pl.ds(zq * BLOCK, BLOCK)
        q = q_ref[rows, :]
        if first:
            m_s[rows, :] = jnp.full((BLOCK, 128), -1e30, F32)
            l_s[rows, :] = jnp.zeros((BLOCK, 128), F32)
            a_s[rows, :] = jnp.zeros((BLOCK, HEAD_DIM), F32)
        else:
            m_s[rows, :] = m_in[rows, :]
            l_s[rows, :] = l_in[rows, :]
            a_s[rows, :] = a_in[rows, :]

        def per_pair(pair, _):
            y_k = where_ref[2 + pair]
            s_two = []
            for core in range(2):
                cores = 0 if core == 0 else 1 - 2 * c_q
                gap = cores * (X * Y * ROWS) + (y_k - y_q) * ROWS
                s_two.append(jnp.where(ahead + gap <= 0, scores(q, pair, zq, core), -1e30))
            accumulate(rows, s_two, pair, zq)

            def per_key(zk, _):
                accumulate(rows, [scores(q, pair, zk, core) for core in range(2)], pair, zk)
                return 0

            lax.fori_loop(0, zq, per_key, 0)
            return 0

        lax.fori_loop(0, n_pairs, per_pair, 0)
        if last:
            total = jnp.sum(l_s[rows, :], axis=1, keepdims=True)
            o_ref[rows, :] = (a_s[rows, :] / total).astype(BF16)
        return 0

    lax.fori_loop(0, Z, per_z, 0)


def attend(where, q, chunks, state, last):
    n_pairs = len(chunks) // 2
    first = state is None
    wide = jax.ShapeDtypeStruct((LOCAL, 128), F32)
    vmem = pl.BlockSpec(memory_space=pltpu.VMEM)
    scratch = [pltpu.VMEM((2 * n_pairs, LOCAL, 2 * HEAD_DIM), BF16)]
    if last:
        out_shape = [jax.ShapeDtypeStruct((LOCAL, HEAD_DIM), BF16)]
        scratch = scratch + [pltpu.VMEM((LOCAL, 128), F32)] * 3
    else:
        out_shape = [wide] * 3
    args = [where, q, *chunks] + ([] if first else list(state))
    pairs = LOCAL * LOCAL * n_pairs * 5 // 4
    return pl.pallas_call(
        functools.partial(attend_body, first, last, n_pairs),
        out_shape=out_shape,
        in_specs=[pl.BlockSpec(memory_space=pltpu.SMEM)] + [vmem] * (len(args) - 1),
        out_specs=[vmem] * len(out_shape),
        scratch_shapes=scratch,
        compiler_params=params(),
        cost_estimate=pl.CostEstimate(
            flops=pairs * 4 * HEAD_DIM, transcendentals=pairs, bytes_accessed=n_pairs * 2 * LOCAL * 512
        ),
    )(*args)


def project_body(attn_ref, wo_ref, tokens_ref, gain_ref, attended_ref, normed_ref, wide_s):
    rows = jnp.concatenate([attn_ref[h] for h in range(HEADS)], axis=1)
    n_k, n_j = wo_ref.shape[0], wo_ref.shape[1]
    for j in range(0, n_j, 2):
        weight = jnp.concatenate(
            [jnp.concatenate([wo_ref[k, j], wo_ref[k, j + 1]], axis=1) for k in range(n_k)], axis=0
        )
        cols = slice(j * 128, (j + 2) * 128)
        share = jnp.dot(rows, weight, preferred_element_type=F32)
        kept = (tokens_ref[:, cols].astype(F32) + share).astype(BF16)
        attended_ref[:, cols] = kept
        wide_s[:, cols] = kept.astype(F32)
    wide = wide_s[...]
    inverse = lax.rsqrt(jnp.mean(wide * wide, axis=1, keepdims=True) + EPS)
    normed_ref[...] = (wide * inverse * gain_ref[...].astype(F32)).astype(BF16)


def project(attn, wo, tokens, gain):
    d = tokens.shape[1]
    vmem = pl.BlockSpec(memory_space=pltpu.VMEM)
    out = jax.ShapeDtypeStruct((ROWS, d), BF16)
    return pl.pallas_call(
        project_body,
        out_shape=[out, out],
        in_specs=[vmem] * 4,
        out_specs=[vmem] * 2,
        scratch_shapes=[pltpu.VMEM((ROWS, d), F32)],
        compiler_params=params(),
        cost_estimate=pl.CostEstimate(
            flops=2 * ROWS * d * d, transcendentals=0, bytes_accessed=2 * d * d
        ),
    )(attn, wo, tokens, gain)


def ffn_body(n_chunks, w_ref, *refs):
    x_refs = refs[:n_chunks]
    o_ref = refs[n_chunks]
    x_s = refs[n_chunks + 1]
    for i in range(n_chunks):
        x_s[i * ROWS : (i + 1) * ROWS, :] = x_refs[i][...]
    tile = 2 * ROWS
    half = w_ref.shape[3]

    def weight(kind, x):
        return jnp.concatenate(
            [w_ref[z * X + x, kind, c] for z in range(Z) for c in range(C)], axis=1
        )

    def per_tile(t, _):
        rows = x_s[pl.ds(t * tile, tile), :]
        acc = None
        for x in range(X):
            nt = (((1,), (1,)), ((), ()))
            gate = lax.dot_general(rows, weight(0, x), nt, preferred_element_type=F32)
            up = lax.dot_general(rows, weight(1, x), nt, preferred_element_type=F32)
            hidden = (gate / (1.0 + jnp.exp(-gate)) * up).astype(BF16)
            part = jnp.dot(hidden, weight(2, x), preferred_element_type=F32)
            acc = part if acc is None else acc + part
        o_ref[pl.ds(t * tile, tile), :] = acc.astype(BF16)
        return 0

    lax.fori_loop(0, n_chunks * ROWS // tile, per_tile, 0)


def ffn(w, chunks):
    d = chunks[0].shape[1]
    n = len(chunks)
    vmem = pl.BlockSpec(memory_space=pltpu.VMEM)
    return pl.pallas_call(
        functools.partial(ffn_body, n),
        out_shape=jax.ShapeDtypeStruct((n * ROWS, d), BF16),
        in_specs=[vmem] * (n + 1),
        out_specs=vmem,
        scratch_shapes=[pltpu.VMEM((n * ROWS, d), BF16)],
        compiler_params=params(),
        cost_estimate=pl.CostEstimate(
            flops=6 * n * ROWS * d * X * w.shape[3],
            transcendentals=n * ROWS * X * w.shape[3],
            bytes_accessed=2 * w.size,
        ),
    )(w, *chunks)


def gather_ring(own):
    half = own.shape[0] // 2
    before = along_y(own, 1)
    after = along_y(own, -1)
    own_c = other_core(own)
    top = along_y(before[:half], 1)
    bottom = along_y(after[half:], -1)
    before_c = other_core(before)
    after_c = other_core(after)
    far = jnp.concatenate([top, bottom], axis=0)
    far_c = other_core(far)
    return (own, own_c), (before, before_c), (after, after_c), (far, far_c)


def reduce_ring(mine, theirs):
    half = ROWS // 2
    got_far = other_core(theirs[3])
    got_near = other_core(theirs[1:3])
    got_own = other_core(theirs[0])

    def add(a, b):
        return a.astype(F32) + b.astype(F32)

    far = add(mine[3], got_far).astype(BF16)
    far_top = along_y(far[:half], 1)
    far_bottom = along_y(far[half:], -1)
    before = add(mine[1], got_near[0])
    after = add(mine[2], got_near[1])
    early_after = along_y(after[half:].astype(BF16), 1)
    early_before = along_y(before[:half].astype(BF16), -1)
    late_after = along_y(add(after[:half], far_top).astype(BF16), 1)
    late_before = along_y(add(before[half:], far_bottom).astype(BF16), -1)
    own = add(mine[0], got_own)
    return jnp.concatenate(
        [
            own[:half] + late_after.astype(F32) + early_before.astype(F32),
            own[half:] + early_after.astype(F32) + late_before.astype(F32),
        ],
        axis=0,
    )


def shards(
    tokens, queries, keys, values, out_weight, norm_gain, gate_weight, up_weight, down_weight
):
    d = tokens.shape[1]
    core = lax.axis_index("c")
    y = lax.axis_index("y")
    group = HEADS // (keys.shape[1] // HEAD_DIM)

    wo = lax.all_gather(out_weight, ("z", "c", "x", "y"), axis=0, tiled=True)
    wo = wo.reshape(Z * C, X * Y, out_weight.shape[0], out_weight.shape[1])

    packed = jnp.stack([gate_weight.T, up_weight.T, down_weight])
    packed = packed.reshape(3, 2, packed.shape[1] // 2, packed.shape[2])
    keep = lax.dynamic_index_in_dim(packed, core, 1, keepdims=False)
    send = lax.dynamic_index_in_dim(packed, 1 - core, 1, keepdims=False)
    got = other_core(send)
    both = jnp.stack([jnp.where(core == 0, keep, got), jnp.where(core == 0, got, keep)], axis=1)
    w = lax.all_gather(both.reshape(-1, both.shape[-1]), ("z", "x"), axis=0, tiled=True)
    w = w.reshape(Z * X, *both.shape)

    def by_head(array, times):
        out = array.reshape(ROWS, -1, 1, HEAD_DIM)
        return jnp.broadcast_to(out, (ROWS, out.shape[1], times, HEAD_DIM)).reshape(ROWS, HEADS, HEAD_DIM)

    kv = jnp.concatenate([by_head(keys, group), by_head(values, group)], axis=2)
    kv = lax.all_to_all(kv.transpose(1, 0, 2), ("z", "x"), split_axis=0, concat_axis=0, tiled=True)
    kv = kv.reshape(LOCAL, 2 * HEAD_DIM)
    q = by_head(queries, 1).transpose(1, 0, 2)
    q = lax.all_to_all(q, ("z", "x"), split_axis=0, concat_axis=0, tiled=True)
    q = q.reshape(LOCAL, HEAD_DIM)

    own, before, after, far = gather_ring(kv)

    def where(*steps):
        return jnp.stack([core, y] + [(y + s) % Y for s in steps]).astype(jnp.int32)

    state = attend(where(0), q, own, None, False)
    state = attend(where(-1, 1), q, before + after, state, False)
    (attn,) = attend(where(2), q, far, state, True)

    attn = lax.all_to_all(
        attn.reshape(HEADS, ROWS, HEAD_DIM), ("z", "x"), split_axis=0, concat_axis=0, tiled=True
    )
    attended, normed = project(attn, wo, tokens, norm_gain.reshape(1, d))

    rows = gather_ring(normed)
    partial = ffn(w, [pair[0] for pair in rows] + [pair[1] for pair in rows])
    partial = partial.reshape(2, 4, ROWS, d)
    layer_out = (attended.astype(F32) + reduce_ring(partial[0], partial[1])).astype(BF16)
    return attended, layer_out


def solution(mesh):
    grid = Mesh(mesh.devices.reshape(Z, C, X, Y), ("z", "c", "x", "y"))
    rows = P(("z", "c", "x", "y"), None)
    block = P(("z", "c"), ("x", "y"))
    return jax.shard_map(
        shards,
        mesh=grid,
        in_specs=(rows, rows, rows, rows, block, P(), block, block, P(("x", "y"), ("z", "c"))),
        out_specs=(rows, rows),
        check_vma=False,
    )
```

```python
import functools

import jax
import jax.numpy as jnp
import numpy as np
from jax import lax
from jax.experimental import pallas as pl
from jax.experimental.pallas import tpu as pltpu
from jax.sharding import Mesh
from jax.sharding import PartitionSpec as P


HEAD_DIM = 128
EPS = 1e-05
ROWS = 128
Z, C, X, Y = 4, 2, 4, 4
HEADS = Z * X
BLOCK = X * ROWS
LOCAL = Z * BLOCK
GROUP = 32
SCALE = float(HEAD_DIM**-0.5 * np.log2(np.e))
F32 = jnp.float32
BF16 = jnp.bfloat16


def params(mib):
    return pltpu.CompilerParams(vmem_limit_bytes=mib * 1024 * 1024)


def along(array, axis, step):
    return lax.ppermute(array, axis, [(i, (i + step) % 4) for i in range(4)])


def along_y(array, step):
    return along(array, "y", step)


def other_core(array):
    return lax.ppermute(array, "c", [(0, 1), (1, 0)])


def attend_body(first, last, n_pairs, where_ref, q_ref, *refs):
    kv_refs = refs[: 2 * n_pairs]
    refs = refs[2 * n_pairs :]
    given = () if first else refs[:3]
    refs = refs[len(given) :]
    if last:
        o_ref, *refs = refs
        kept = ()
    else:
        kept = refs[:3]
        refs = refs[3:]
    m_s, l_s, a_s, arrived, left = refs
    held = (m_s, l_s, a_s)

    def rows_of(zq):
        return pl.ds(pl.multiple_of(zq * BLOCK, BLOCK), BLOCK)

    def arriving(i, zq):
        rows = rows_of(zq)
        return pltpu.make_async_copy(given[i].at[rows], held[i].at[rows], arrived.at[i, zq])

    def leaving(i, zq):
        rows = rows_of(zq)
        return pltpu.make_async_copy(held[i].at[rows], kept[i].at[rows], left.at[i, zq])

    for zq in range(Z):
        for i in range(len(given)):
            arriving(i, zq).start()
    c_q = where_ref[0]
    y_q = where_ref[1]
    lanes = BLOCK // 128

    def accumulate(zq, zk):
        start = pl.multiple_of(zq * BLOCK, BLOCK)
        keys = pl.ds(pl.multiple_of(zk * BLOCK, BLOCK), BLOCK)
        q = q_ref[pl.ds(start, BLOCK), :]
        scores = [
            lax.dot_general(
                q, kv_refs[i][keys, :HEAD_DIM], (((1,), (1,)), ((), ())), preferred_element_type=F32
            )
            for i in range(2 * n_pairs)
        ]
        ahead = lax.broadcasted_iota(jnp.int32, (GROUP, 128), 1) - lax.broadcasted_iota(
            jnp.int32, (GROUP, 128), 0
        )
        probs = [[] for _ in range(2 * n_pairs)]
        for low in range(0, BLOCK, GROUP):
            rows = pl.ds(start + low, GROUP)
            tiles = []
            for i in range(2 * n_pairs):
                for lane in range(lanes):
                    tile = scores[i][low : low + GROUP, lane * 128 : (lane + 1) * 128] * SCALE
                    cores = C * (zk - zq) + (0 if i % 2 == 0 else 1 - 2 * c_q)
                    gap = cores * (X * Y * ROWS) + (where_ref[2 + i // 2] - y_q) * ROWS
                    gap = gap + (lane - low // ROWS) * (Y * ROWS) - low % ROWS
                    tiles.append(jnp.where(ahead <= -gap, tile, -1e30))
            m_old = m_s[rows, :]
            peak = jnp.max(functools.reduce(jnp.maximum, tiles), axis=1, keepdims=True)
            m_new = jnp.maximum(m_old, jnp.broadcast_to(peak, m_old.shape))
            alpha = jnp.exp2(m_old - m_new)
            terms = [jnp.exp2(tile - m_new) for tile in tiles]
            m_s[rows, :] = m_new
            l_s[rows, :] = l_s[rows, :] * alpha + functools.reduce(jnp.add, terms)
            a_s[rows, :] = a_s[rows, :] * alpha
            for i in range(2 * n_pairs):
                mine = [t.astype(BF16) for t in terms[i * lanes : (i + 1) * lanes]]
                probs[i].append(jnp.concatenate(mine, axis=1))
        mixed = None
        for i in range(2 * n_pairs):
            p = jnp.concatenate(probs[i], axis=0)
            part = jnp.dot(p, kv_refs[i][keys, HEAD_DIM:], preferred_element_type=F32)
            mixed = part if mixed is None else mixed + part
        a_s[pl.ds(start, BLOCK), :] = a_s[pl.ds(start, BLOCK), :] + mixed

    def per_z(zq, _):
        rows = pl.ds(pl.multiple_of(zq * BLOCK, BLOCK), BLOCK)
        if first:
            m_s[rows, :] = jnp.full((BLOCK, 128), -1e30, F32)
            l_s[rows, :] = jnp.zeros((BLOCK, 128), F32)
            a_s[rows, :] = jnp.zeros((BLOCK, HEAD_DIM), F32)
        else:
            for i in range(3):
                arriving(i, zq).wait()

        def per_key(zk, _):
            accumulate(zq, zk)
            return 0

        lax.fori_loop(0, zq + 1, per_key, 0)
        if last:
            total = jnp.sum(l_s[rows, :], axis=1, keepdims=True)
            o_ref[rows, :] = (a_s[rows, :] / total).astype(BF16)
        for i in range(len(kept)):
            leaving(i, zq).start()
        return 0

    lax.fori_loop(0, Z, per_z, 0)
    for zq in range(Z):
        for i in range(len(kept)):
            leaving(i, zq).wait()


def attend(where, q, chunks, state, last):
    n_pairs = len(chunks) // 2
    first = state is None
    wide = pltpu.HBM((LOCAL, 128), F32)
    vmem = pl.BlockSpec(memory_space=pltpu.VMEM)
    hbm = pl.BlockSpec(memory_space=pltpu.HBM)
    args = [where, q, *chunks]
    if not first:
        args += [pltpu.with_memory_space_constraint(a, pltpu.HBM) for a in state]
    n_vmem = 1 + len(chunks)
    pairs = LOCAL * LOCAL * n_pairs * 5 // 4
    return pl.pallas_call(
        functools.partial(attend_body, first, last, n_pairs),
        out_shape=jax.ShapeDtypeStruct((LOCAL, HEAD_DIM), BF16) if last else [wide] * 3,
        in_specs=[pl.BlockSpec(memory_space=pltpu.SMEM)]
        + [vmem] * n_vmem
        + [hbm] * (len(args) - 1 - n_vmem),
        out_specs=vmem if last else [hbm] * 3,
        scratch_shapes=[pltpu.VMEM((LOCAL, 128), F32)] * 3
        + [pltpu.SemaphoreType.DMA((3, Z))] * 2,
        compiler_params=params(22),
        cost_estimate=pl.CostEstimate(
            flops=pairs * 4 * HEAD_DIM, transcendentals=pairs, bytes_accessed=n_pairs * 2 * LOCAL * 512
        ),
    )(*args)


def project_body(where_ref, attn_ref, tokens_ref, gain_ref, *refs):
    wo_refs = refs[:8]
    attended_ref, normed_ref, wide_s = refs[8:]
    core, z_own, x_own = where_ref[0], where_ref[1], where_ref[2]
    heads = []
    for c in (core, 1 - core):
        for z in range(Z):
            for e in range(2):
                heads.append(attn_ref[2 * (2 * ((z_own - z) % Z) + c) + e])
    rows = jnp.concatenate(heads, axis=1)
    for i in range(Y):
        y = where_ref[3 + i]
        for x in range(0, X, 2):
            weight = jnp.concatenate(
                [
                    jnp.concatenate([ref[z * X + x], ref[z * X + x + 1]], axis=1)
                    for ref in wo_refs[2 * i : 2 * i + 2]
                    for z in range(Z)
                ],
                axis=0,
            )
            share = jnp.dot(rows, weight, preferred_element_type=F32)
            for side in range(2):
                column = (x_own - x - side) % X * Y + y
                cols = pl.ds(pl.multiple_of(column * 128, 128), 128)
                part = share[:, side * 128 : (side + 1) * 128]
                kept = (tokens_ref[:, cols].astype(F32) + part).astype(BF16)
                attended_ref[:, cols] = kept
                wide_s[:, cols] = kept.astype(F32)
    wide = wide_s[...]
    inverse = lax.rsqrt(jnp.mean(wide * wide, axis=1, keepdims=True) + EPS)
    normed_ref[...] = (wide * inverse * gain_ref[...].astype(F32)).astype(BF16)


def project(where, attn, wo, tokens, gain):
    d = tokens.shape[1]
    vmem = pl.BlockSpec(memory_space=pltpu.VMEM)
    out = jax.ShapeDtypeStruct((ROWS, d), BF16)
    return pl.pallas_call(
        project_body,
        out_shape=[out, out],
        in_specs=[pl.BlockSpec(memory_space=pltpu.SMEM)] + [vmem] * (3 + len(wo)),
        out_specs=[vmem] * 2,
        scratch_shapes=[pltpu.VMEM((ROWS, d), F32)],
        compiler_params=params(14),
        cost_estimate=pl.CostEstimate(
            flops=2 * ROWS * d * d, transcendentals=0, bytes_accessed=2 * d * d
        ),
    )(where, attn, tokens, gain, *wo)


def ffn_body(n_chunks, w_ref, *refs):
    x_refs = refs[:n_chunks]
    o_ref = refs[n_chunks]
    x_s = refs[n_chunks + 1]
    for i in range(n_chunks):
        x_s[i * ROWS : (i + 1) * ROWS, :] = x_refs[i][...]
    tile = 2 * ROWS

    def weight(kind, x):
        return jnp.concatenate(
            [w_ref[z * X + x, kind, c] for z in range(Z) for c in range(C)], axis=1
        )

    def per_tile(t, _):
        rows = x_s[pl.ds(pl.multiple_of(t * tile, tile), tile), :]
        acc = None
        for x in range(X):
            nt = (((1,), (1,)), ((), ()))
            gate = lax.dot_general(rows, weight(0, x), nt, preferred_element_type=F32)
            up = lax.dot_general(rows, weight(1, x), nt, preferred_element_type=F32)
            hidden = (gate / (1.0 + jnp.exp(-gate)) * up).astype(BF16)
            part = jnp.dot(hidden, weight(2, x), preferred_element_type=F32)
            acc = part if acc is None else acc + part
        o_ref[pl.ds(pl.multiple_of(t * tile, tile), tile), :] = acc.astype(BF16)
        return 0

    lax.fori_loop(0, n_chunks * ROWS // tile, per_tile, 0)


def ffn(w, chunks):
    d = chunks[0].shape[1]
    n = len(chunks)
    vmem = pl.BlockSpec(memory_space=pltpu.VMEM)
    return pl.pallas_call(
        functools.partial(ffn_body, n),
        out_shape=jax.ShapeDtypeStruct((n * ROWS, d), BF16),
        in_specs=[vmem] * (n + 1),
        out_specs=vmem,
        scratch_shapes=[pltpu.VMEM((n * ROWS, d), BF16)],
        compiler_params=params(26),
        cost_estimate=pl.CostEstimate(
            flops=6 * n * ROWS * d * X * w.shape[3],
            transcendentals=n * ROWS * X * w.shape[3],
            bytes_accessed=2 * w.size,
        ),
    )(w, *chunks)


def gather_near(own):
    before = along_y(own, 1)
    after = along_y(own, -1)
    return other_core(own), (before, other_core(before)), (after, other_core(after))


def gather_far(before, after):
    half = before.shape[0] // 2
    top = along_y(before[:half], 1)
    bottom = along_y(after[half:], -1)
    far = jnp.concatenate([top, bottom], axis=0)
    return far, other_core(far)


def wide_add(a, b):
    return a.astype(F32) + b.astype(F32)


def shards(
    tokens, queries, keys, values, out_weight, norm_gain, gate_weight, up_weight, down_weight
):
    d = tokens.shape[1]
    core = lax.axis_index("c")
    y = lax.axis_index("y")
    group = HEADS // (keys.shape[1] // HEAD_DIM)

    def by_head(array, times):
        out = array.reshape(ROWS, -1, 1, HEAD_DIM)
        out = jnp.broadcast_to(out, (ROWS, out.shape[1], times, HEAD_DIM))
        return out.reshape(ROWS, HEADS, HEAD_DIM)

    def regroup(array):
        return lax.all_to_all(array, ("z", "x"), split_axis=0, concat_axis=0, tiled=True)

    kv = jnp.concatenate([by_head(keys, group), by_head(values, group)], axis=2)
    kv = regroup(kv.transpose(1, 0, 2)).reshape(LOCAL, 2 * HEAD_DIM)
    kv_c, before, after = gather_near(kv)

    wo = jnp.stack([out_weight] + [along(out_weight, "x", i) for i in range(1, X)])
    wo = lax.optimization_barrier(wo)
    wo = jnp.stack([wo] + [along(wo, "z", i) for i in range(1, Z)])
    wo = wo.reshape(Z * X, *out_weight.shape)

    q = regroup(by_head(queries, 1).transpose(1, 0, 2)).reshape(LOCAL, HEAD_DIM)

    packed = jnp.stack([gate_weight.T, up_weight.T, down_weight])
    packed = packed.reshape(3, 2, packed.shape[1] // 2, packed.shape[2])
    keep = lax.dynamic_index_in_dim(packed, core, 1, keepdims=False)
    send = lax.dynamic_index_in_dim(packed, 1 - core, 1, keepdims=False)
    got = other_core(send)
    both = jnp.stack([jnp.where(core == 0, keep, got), jnp.where(core == 0, got, keep)], axis=1)
    w = lax.all_gather(both.reshape(-1, both.shape[-1]), ("z", "x"), axis=0, tiled=True)
    w = w.reshape(Z * X, *both.shape)

    def where(*steps):
        return jnp.stack([core, y] + [(y + s) % Y for s in steps]).astype(jnp.int32)

    state = attend(where(0), q, [kv, kv_c], None, False)
    far = gather_far(before[0], after[0])
    state = attend(where(-1, 1), q, [*before, *after], state, False)
    attn = attend(where(2), q, far, state, True)

    wo_c, wo_before, wo_after = gather_near(wo)
    wo_far = gather_far(wo_before[0], wo_after[0])
    attn = regroup(attn.reshape(HEADS, ROWS, HEAD_DIM))
    attn, w = lax.optimization_barrier((attn, w))
    attended, normed = project(
        jnp.stack(
            [core, lax.axis_index("z"), lax.axis_index("x")]
            + [(y + s) % Y for s in (0, -1, 1, 2)]
        ).astype(jnp.int32),
        attn,
        [wo, wo_c, *wo_before, *wo_after, *wo_far],
        tokens,
        norm_gain.reshape(1, d),
    )

    normed_c, before, after = gather_near(normed)
    own_part = ffn(w, [normed, normed_c])
    far = gather_far(before[0], after[0])
    near_part = ffn(w, [before[0], after[0], before[1], after[1]])
    far_part = ffn(w, far)

    half = ROWS // 2
    got_own = other_core(own_part[ROWS:])
    got_near = other_core(near_part[2 * ROWS :])
    before = wide_add(near_part[:ROWS], got_near[:ROWS])
    after = wide_add(near_part[ROWS : 2 * ROWS], got_near[ROWS:])
    early_after = along_y(after[half:].astype(BF16), 1)
    early_before = along_y(before[:half].astype(BF16), -1)
    far = wide_add(far_part[:ROWS], other_core(far_part[ROWS:])).astype(BF16)
    far_top = along_y(far[:half], 1)
    far_bottom = along_y(far[half:], -1)
    far_top, far_bottom = lax.optimization_barrier((far_top, far_bottom))
    late_after = along_y(wide_add(after[:half], far_top).astype(BF16), 1)
    late_before = along_y(wide_add(before[half:], far_bottom).astype(BF16), -1)
    own = wide_add(own_part[:ROWS], got_own)
    total = jnp.concatenate(
        [
            own[:half] + wide_add(late_after, early_before),
            own[half:] + wide_add(early_after, late_before),
        ],
        axis=0,
    )
    return attended, (attended.astype(F32) + total).astype(BF16)


def solution(mesh):
    grid = Mesh(mesh.devices.reshape(Z, C, X, Y), ("z", "c", "x", "y"))
    rows = P(("z", "c", "x", "y"), None)
    block = P(("z", "c"), ("x", "y"))
    return jax.shard_map(
        shards,
        mesh=grid,
        in_specs=(rows, rows, rows, rows, block, P(), block, block, P(("x", "y"), ("z", "c"))),
        out_specs=(rows, rows),
        check_vma=False,
    )
```

```python
import functools

import jax
import jax.numpy as jnp
import numpy as np
from jax import lax
from jax.experimental import pallas as pl
from jax.experimental.pallas import tpu as pltpu
from jax.sharding import Mesh
from jax.sharding import PartitionSpec as P


HEAD_DIM = 128
EPS = 1e-05
ROWS = 128
Z, C, X, Y = 4, 2, 4, 4
HEADS = Z * X
BLOCK = X * ROWS
LOCAL = Z * BLOCK
GROUP = 32
SCALE = float(HEAD_DIM**-0.5 * np.log2(np.e))
F32 = jnp.float32
BF16 = jnp.bfloat16


def params(mib):
    return pltpu.CompilerParams(vmem_limit_bytes=mib * 1024 * 1024)


def along(array, axis, step):
    return lax.ppermute(array, axis, [(i, (i + step) % 4) for i in range(4)])


def along_y(array, step):
    return along(array, "y", step)


def other_core(array):
    return lax.ppermute(array, "c", [(0, 1), (1, 0)])


def by_head_body(keys_ref, values_ref, o_ref):
    n_kv = keys_ref.shape[1] // HEAD_DIM
    for h in range(HEADS):
        g = h * n_kv // HEADS
        cols = slice(g * HEAD_DIM, (g + 1) * HEAD_DIM)
        o_ref[h, :, :HEAD_DIM] = keys_ref[:, cols]
        o_ref[h, :, HEAD_DIM:] = values_ref[:, cols]


def by_head(keys, values):
    vmem = pl.BlockSpec(memory_space=pltpu.VMEM)
    return pl.pallas_call(
        by_head_body,
        out_shape=jax.ShapeDtypeStruct((HEADS, ROWS, 2 * HEAD_DIM), BF16),
        in_specs=[vmem] * 2,
        out_specs=vmem,
        compiler_params=params(8),
    )(keys, values)


def attend_body(first, last, n_pairs, where_ref, q_ref, *refs):
    kv_refs = refs[: 2 * n_pairs]
    refs = refs[2 * n_pairs :]
    given = () if first else refs[:3]
    refs = refs[len(given) :]
    if last:
        o_ref, *refs = refs
        kept = ()
    else:
        kept = refs[:3]
        refs = refs[3:]
    m_s, l_s, a_s, arrived, left = refs
    held = (m_s, l_s, a_s)

    def rows_of(zq):
        return pl.ds(pl.multiple_of(zq * BLOCK, BLOCK), BLOCK)

    def arriving(i, zq):
        rows = rows_of(zq)
        return pltpu.make_async_copy(given[i].at[rows], held[i].at[rows], arrived.at[i, zq])

    def leaving(i, zq):
        rows = rows_of(zq)
        return pltpu.make_async_copy(held[i].at[rows], kept[i].at[rows], left.at[i, zq])

    for zq in range(Z):
        for i in range(len(given)):
            arriving(i, zq).start()
    c_q = where_ref[0]
    y_q = where_ref[1]
    lanes = BLOCK // 128

    def accumulate(zq, zk):
        start = pl.multiple_of(zq * BLOCK, BLOCK)
        keys = pl.ds(pl.multiple_of(zk * BLOCK, BLOCK), BLOCK)
        q = q_ref[pl.ds(start, BLOCK), :]
        scores = [
            lax.dot_general(
                q, kv_refs[i][keys, :HEAD_DIM], (((1,), (1,)), ((), ())), preferred_element_type=F32
            )
            for i in range(2 * n_pairs)
        ]
        ahead = lax.broadcasted_iota(jnp.int32, (GROUP, 128), 1) - lax.broadcasted_iota(
            jnp.int32, (GROUP, 128), 0
        )
        probs = [[] for _ in range(2 * n_pairs)]
        for low in range(0, BLOCK, GROUP):
            rows = pl.ds(start + low, GROUP)
            tiles = []
            for i in range(2 * n_pairs):
                for lane in range(lanes):
                    tile = scores[i][low : low + GROUP, lane * 128 : (lane + 1) * 128] * SCALE
                    cores = C * (zk - zq) + (0 if i % 2 == 0 else 1 - 2 * c_q)
                    gap = cores * (X * Y * ROWS) + (where_ref[2 + i // 2] - y_q) * ROWS
                    gap = gap + (lane - low // ROWS) * (Y * ROWS) - low % ROWS
                    tiles.append(jnp.where(ahead <= -gap, tile, -1e30))
            m_old = m_s[rows, :]
            peak = jnp.max(functools.reduce(jnp.maximum, tiles), axis=1, keepdims=True)
            m_new = jnp.maximum(m_old, jnp.broadcast_to(peak, m_old.shape))
            alpha = jnp.exp2(m_old - m_new)
            terms = [jnp.exp2(tile - m_new) for tile in tiles]
            m_s[rows, :] = m_new
            l_s[rows, :] = l_s[rows, :] * alpha + functools.reduce(jnp.add, terms)
            a_s[rows, :] = a_s[rows, :] * alpha
            for i in range(2 * n_pairs):
                mine = [t.astype(BF16) for t in terms[i * lanes : (i + 1) * lanes]]
                probs[i].append(jnp.concatenate(mine, axis=1))
        mixed = None
        for i in range(2 * n_pairs):
            p = jnp.concatenate(probs[i], axis=0)
            part = jnp.dot(p, kv_refs[i][keys, HEAD_DIM:], preferred_element_type=F32)
            mixed = part if mixed is None else mixed + part
        a_s[pl.ds(start, BLOCK), :] = a_s[pl.ds(start, BLOCK), :] + mixed

    def per_z(zq, _):
        rows = pl.ds(pl.multiple_of(zq * BLOCK, BLOCK), BLOCK)
        if first:
            m_s[rows, :] = jnp.full((BLOCK, 128), -1e30, F32)
            l_s[rows, :] = jnp.zeros((BLOCK, 128), F32)
            a_s[rows, :] = jnp.zeros((BLOCK, HEAD_DIM), F32)
        else:
            for i in range(3):
                arriving(i, zq).wait()

        def per_key(zk, _):
            accumulate(zq, zk)
            return 0

        lax.fori_loop(0, zq + 1, per_key, 0)
        if last:
            total = jnp.sum(l_s[rows, :], axis=1, keepdims=True)
            o_ref[rows, :] = (a_s[rows, :] / total).astype(BF16)
        for i in range(len(kept)):
            leaving(i, zq).start()
        return 0

    lax.fori_loop(0, Z, per_z, 0)
    for zq in range(Z):
        for i in range(len(kept)):
            leaving(i, zq).wait()


def attend(where, q, chunks, state, last):
    n_pairs = len(chunks) // 2
    first = state is None
    wide = pltpu.HBM((LOCAL, 128), F32)
    vmem = pl.BlockSpec(memory_space=pltpu.VMEM)
    hbm = pl.BlockSpec(memory_space=pltpu.HBM)
    args = [where, q, *chunks]
    if not first:
        args += [pltpu.with_memory_space_constraint(a, pltpu.HBM) for a in state]
    n_vmem = 1 + len(chunks)
    pairs = LOCAL * LOCAL * n_pairs * 5 // 4
    return pl.pallas_call(
        functools.partial(attend_body, first, last, n_pairs),
        out_shape=jax.ShapeDtypeStruct((LOCAL, HEAD_DIM), BF16) if last else [wide] * 3,
        in_specs=[pl.BlockSpec(memory_space=pltpu.SMEM)]
        + [vmem] * n_vmem
        + [hbm] * (len(args) - 1 - n_vmem),
        out_specs=vmem if last else [hbm] * 3,
        scratch_shapes=[pltpu.VMEM((LOCAL, 128), F32)] * 3
        + [pltpu.SemaphoreType.DMA((3, Z))] * 2,
        compiler_params=params(22),
        cost_estimate=pl.CostEstimate(
            flops=pairs * 4 * HEAD_DIM, transcendentals=pairs, bytes_accessed=n_pairs * 2 * LOCAL * 512
        ),
    )(*args)


def project_body(where_ref, attn_ref, tokens_ref, gain_ref, *refs):
    wo_refs = refs[:8]
    attended_ref, normed_ref, wide_s = refs[8:]
    core, z_own, x_own = where_ref[0], where_ref[1], where_ref[2]
    heads = []
    for c in (core, 1 - core):
        for z in range(Z):
            for e in range(2):
                heads.append(attn_ref[2 * (2 * ((z_own - z) % Z) + c) + e])
    rows = jnp.concatenate(heads, axis=1)
    for i in range(Y):
        y = where_ref[3 + i]
        for x in range(0, X, 2):
            weight = jnp.concatenate(
                [
                    jnp.concatenate([ref[z * X + x], ref[z * X + x + 1]], axis=1)
                    for ref in wo_refs[2 * i : 2 * i + 2]
                    for z in range(Z)
                ],
                axis=0,
            )
            share = jnp.dot(rows, weight, preferred_element_type=F32)
            for side in range(2):
                column = (x_own - x - side) % X * Y + y
                cols = pl.ds(pl.multiple_of(column * 128, 128), 128)
                part = share[:, side * 128 : (side + 1) * 128]
                kept = (tokens_ref[:, cols].astype(F32) + part).astype(BF16)
                attended_ref[:, cols] = kept
                wide_s[:, cols] = kept.astype(F32)
    wide = wide_s[...]
    inverse = lax.rsqrt(jnp.mean(wide * wide, axis=1, keepdims=True) + EPS)
    normed_ref[...] = (wide * inverse * gain_ref[...].astype(F32)).astype(BF16)


def project(where, attn, wo, tokens, gain):
    d = tokens.shape[1]
    vmem = pl.BlockSpec(memory_space=pltpu.VMEM)
    out = jax.ShapeDtypeStruct((ROWS, d), BF16)
    return pl.pallas_call(
        project_body,
        out_shape=[out, out],
        in_specs=[pl.BlockSpec(memory_space=pltpu.SMEM)] + [vmem] * (3 + len(wo)),
        out_specs=[vmem] * 2,
        scratch_shapes=[pltpu.VMEM((ROWS, d), F32)],
        compiler_params=params(14),
        cost_estimate=pl.CostEstimate(
            flops=2 * ROWS * d * d, transcendentals=0, bytes_accessed=2 * d * d
        ),
    )(where, attn, tokens, gain, *wo)


def ffn_body(n_chunks, w_ref, *refs):
    x_refs = refs[:n_chunks]
    o_ref = refs[n_chunks]
    x_s = refs[n_chunks + 1]
    for i in range(n_chunks):
        x_s[i * ROWS : (i + 1) * ROWS, :] = x_refs[i][...]
    tile = 2 * ROWS

    def weight(kind, x):
        return jnp.concatenate(
            [w_ref[z * X + x, kind, c] for z in range(Z) for c in range(C)], axis=1
        )

    def per_tile(t, _):
        rows = x_s[pl.ds(pl.multiple_of(t * tile, tile), tile), :]
        acc = None
        for x in range(X):
            nt = (((1,), (1,)), ((), ()))
            gate = lax.dot_general(rows, weight(0, x), nt, preferred_element_type=F32)
            up = lax.dot_general(rows, weight(1, x), nt, preferred_element_type=F32)
            hidden = (gate / (1.0 + jnp.exp(-gate)) * up).astype(BF16)
            part = jnp.dot(hidden, weight(2, x), preferred_element_type=F32)
            acc = part if acc is None else acc + part
        o_ref[pl.ds(pl.multiple_of(t * tile, tile), tile), :] = acc.astype(BF16)
        return 0

    lax.fori_loop(0, n_chunks * ROWS // tile, per_tile, 0)


def ffn(w, chunks):
    d = chunks[0].shape[1]
    n = len(chunks)
    vmem = pl.BlockSpec(memory_space=pltpu.VMEM)
    return pl.pallas_call(
        functools.partial(ffn_body, n),
        out_shape=jax.ShapeDtypeStruct((n * ROWS, d), BF16),
        in_specs=[vmem] * (n + 1),
        out_specs=vmem,
        scratch_shapes=[pltpu.VMEM((n * ROWS, d), BF16)],
        compiler_params=params(26),
        cost_estimate=pl.CostEstimate(
            flops=6 * n * ROWS * d * X * w.shape[3],
            transcendentals=n * ROWS * X * w.shape[3],
            bytes_accessed=2 * w.size,
        ),
    )(w, *chunks)


def gather_near(own):
    before = along_y(own, 1)
    after = along_y(own, -1)
    return other_core(own), (before, other_core(before)), (after, other_core(after))


def gather_far(before, after):
    half = before.shape[0] // 2
    top = along_y(before[:half], 1)
    bottom = along_y(after[half:], -1)
    far = jnp.concatenate([top, bottom], axis=0)
    return far, other_core(far)


def wide_add(a, b):
    return a.astype(F32) + b.astype(F32)


def shards(
    tokens, queries, keys, values, out_weight, norm_gain, gate_weight, up_weight, down_weight
):
    d = tokens.shape[1]
    core = lax.axis_index("c")
    y = lax.axis_index("y")

    def regroup(array):
        return lax.all_to_all(array, ("z", "x"), split_axis=0, concat_axis=0, tiled=True)

    kv = by_head(keys, values)
    kv = regroup(kv).reshape(LOCAL, 2 * HEAD_DIM)
    kv_c, before, after = gather_near(kv)

    wo = jnp.stack([out_weight] + [along(out_weight, "x", i) for i in range(1, X)])
    wo = lax.optimization_barrier(wo)
    wo = jnp.stack([wo] + [along(wo, "z", i) for i in range(1, Z)])
    wo = wo.reshape(Z * X, *out_weight.shape)

    q = queries.reshape(ROWS, HEADS, HEAD_DIM).transpose(1, 0, 2)
    q = regroup(q).reshape(LOCAL, HEAD_DIM)

    packed = jnp.stack([gate_weight.T, up_weight.T, down_weight])
    packed = packed.reshape(3, 2, packed.shape[1] // 2, packed.shape[2])
    keep = lax.dynamic_index_in_dim(packed, core, 1, keepdims=False)
    send = lax.dynamic_index_in_dim(packed, 1 - core, 1, keepdims=False)
    got = other_core(send)
    both = jnp.stack([jnp.where(core == 0, keep, got), jnp.where(core == 0, got, keep)], axis=1)
    w = lax.all_gather(both.reshape(-1, both.shape[-1]), ("z", "x"), axis=0, tiled=True)
    w = w.reshape(Z * X, *both.shape)

    def where(*steps):
        return jnp.stack([core, y] + [(y + s) % Y for s in steps]).astype(jnp.int32)

    state = attend(where(0), q, [kv, kv_c], None, False)
    far = gather_far(before[0], after[0])
    state = attend(where(-1, 1), q, [*before, *after], state, False)
    attn = attend(where(2), q, far, state, True)

    wo_c, wo_before, wo_after = gather_near(wo)
    wo_far = gather_far(wo_before[0], wo_after[0])
    attn = regroup(attn.reshape(HEADS, ROWS, HEAD_DIM))
    attn, w = lax.optimization_barrier((attn, w))
    attended, normed = project(
        jnp.stack(
            [core, lax.axis_index("z"), lax.axis_index("x")]
            + [(y + s) % Y for s in (0, -1, 1, 2)]
        ).astype(jnp.int32),
        attn,
        [wo, wo_c, *wo_before, *wo_after, *wo_far],
        tokens,
        norm_gain.reshape(1, d),
    )

    normed_c, before, after = gather_near(normed)
    own_part = ffn(w, [normed, normed_c])
    far = gather_far(before[0], after[0])
    near_part = ffn(w, [before[0], after[0], before[1], after[1]])
    far_part = ffn(w, far)

    half = ROWS // 2
    got_own = other_core(own_part[ROWS:])
    got_near = other_core(near_part[2 * ROWS :])
    before = wide_add(near_part[:ROWS], got_near[:ROWS])
    after = wide_add(near_part[ROWS : 2 * ROWS], got_near[ROWS:])
    early_after = along_y(after[half:].astype(BF16), 1)
    early_before = along_y(before[:half].astype(BF16), -1)
    far = wide_add(far_part[:ROWS], other_core(far_part[ROWS:])).astype(BF16)
    far_top = along_y(far[:half], 1)
    far_bottom = along_y(far[half:], -1)
    far_top, far_bottom = lax.optimization_barrier((far_top, far_bottom))
    late_after = along_y(wide_add(after[:half], far_top).astype(BF16), 1)
    late_before = along_y(wide_add(before[half:], far_bottom).astype(BF16), -1)
    own = wide_add(own_part[:ROWS], got_own)
    total = jnp.concatenate(
        [
            own[:half] + wide_add(late_after, early_before),
            own[half:] + wide_add(early_after, late_before),
        ],
        axis=0,
    )
    return attended, (attended.astype(F32) + total).astype(BF16)


def solution(mesh):
    grid = Mesh(mesh.devices.reshape(Z, C, X, Y), ("z", "c", "x", "y"))
    rows = P(("z", "c", "x", "y"), None)
    block = P(("z", "c"), ("x", "y"))
    return jax.shard_map(
        shards,
        mesh=grid,
        in_specs=(rows, rows, rows, rows, block, P(), block, block, P(("x", "y"), ("z", "c"))),
        out_specs=(rows, rows),
        check_vma=False,
    )
```

```python
import functools

import jax
import jax.numpy as jnp
import numpy as np
from jax import lax
from jax.experimental import pallas as pl
from jax.experimental.pallas import tpu as pltpu
from jax.sharding import Mesh
from jax.sharding import PartitionSpec as P


HEAD_DIM = 128
EPS = 1e-05
ROWS = 128
Z, C, X, Y = 4, 2, 4, 4
HEADS = Z * X
BLOCK = X * ROWS
LOCAL = Z * BLOCK
GROUP = 32
SCALE = float(HEAD_DIM**-0.5 * np.log2(np.e))
F32 = jnp.float32
BF16 = jnp.bfloat16


def params(mib):
    return pltpu.CompilerParams(vmem_limit_bytes=mib * 1024 * 1024)


def along(array, axis, step):
    return lax.ppermute(array, axis, [(i, (i + step) % 4) for i in range(4)])


def along_y(array, step):
    return along(array, "y", step)


def other_core(array):
    return lax.ppermute(array, "c", [(0, 1), (1, 0)])


def by_head_body(keys_ref, values_ref, o_ref):
    n_kv = keys_ref.shape[1] // HEAD_DIM
    for h in range(HEADS):
        g = h * n_kv // HEADS
        cols = slice(g * HEAD_DIM, (g + 1) * HEAD_DIM)
        o_ref[h, :, :HEAD_DIM] = keys_ref[:, cols]
        o_ref[h, :, HEAD_DIM:] = values_ref[:, cols]


def by_head(keys, values):
    vmem = pl.BlockSpec(memory_space=pltpu.VMEM)
    return pl.pallas_call(
        by_head_body,
        out_shape=jax.ShapeDtypeStruct((HEADS, ROWS, 2 * HEAD_DIM), BF16),
        in_specs=[vmem] * 2,
        out_specs=vmem,
        compiler_params=params(8),
    )(keys, values)


def attend_body(first, last, n_pairs, zs, where_ref, q_ref, *refs):
    kv_refs = refs[: 2 * n_pairs]
    refs = refs[2 * n_pairs :]
    given = () if first else refs[:3]
    refs = refs[len(given) :]
    if last:
        o_ref, *refs = refs
        kept = ()
    else:
        kept = refs[:3]
        refs = refs[3:]
    m_s, l_s, a_s, arrived, left = refs
    held = (m_s, l_s, a_s)

    def rows_of(zq):
        return pl.ds(pl.multiple_of(zq * BLOCK, BLOCK), BLOCK)

    def arriving(i, zq):
        rows = rows_of(zq)
        return pltpu.make_async_copy(given[i].at[rows], held[i].at[rows], arrived.at[i, zq])

    def leaving(i, zq):
        rows = rows_of(zq)
        return pltpu.make_async_copy(held[i].at[rows], kept[i].at[rows], left.at[i, zq])

    for zq in range(*zs):
        for i in range(len(given)):
            arriving(i, zq).start()
    c_q = where_ref[0]
    y_q = where_ref[1]
    lanes = BLOCK // 128

    def accumulate(zq, zk):
        start = pl.multiple_of(zq * BLOCK, BLOCK)
        keys = pl.ds(pl.multiple_of(zk * BLOCK, BLOCK), BLOCK)
        q = q_ref[pl.ds(start, BLOCK), :]
        scores = [
            lax.dot_general(
                q, kv_refs[i][keys, :HEAD_DIM], (((1,), (1,)), ((), ())), preferred_element_type=F32
            )
            for i in range(2 * n_pairs)
        ]
        ahead = lax.broadcasted_iota(jnp.int32, (GROUP, 128), 1) - lax.broadcasted_iota(
            jnp.int32, (GROUP, 128), 0
        )
        probs = [[] for _ in range(2 * n_pairs)]
        for low in range(0, BLOCK, GROUP):
            rows = pl.ds(start + low, GROUP)
            tiles = []
            for i in range(2 * n_pairs):
                for lane in range(lanes):
                    tile = scores[i][low : low + GROUP, lane * 128 : (lane + 1) * 128] * SCALE
                    cores = C * (zk - zq) + (0 if i % 2 == 0 else 1 - 2 * c_q)
                    gap = cores * (X * Y * ROWS) + (where_ref[2 + i // 2] - y_q) * ROWS
                    gap = gap + (lane - low // ROWS) * (Y * ROWS) - low % ROWS
                    tiles.append(jnp.where(ahead <= -gap, tile, -1e30))
            m_old = m_s[rows, :]
            peak = jnp.max(functools.reduce(jnp.maximum, tiles), axis=1, keepdims=True)
            m_new = jnp.maximum(m_old, jnp.broadcast_to(peak, m_old.shape))
            alpha = jnp.exp2(m_old - m_new)
            terms = [jnp.exp2(tile - m_new) for tile in tiles]
            m_s[rows, :] = m_new
            l_s[rows, :] = l_s[rows, :] * alpha + functools.reduce(jnp.add, terms)
            a_s[rows, :] = a_s[rows, :] * alpha
            for i in range(2 * n_pairs):
                mine = [t.astype(BF16) for t in terms[i * lanes : (i + 1) * lanes]]
                probs[i].append(jnp.concatenate(mine, axis=1))
        mixed = None
        for i in range(2 * n_pairs):
            p = jnp.concatenate(probs[i], axis=0)
            part = jnp.dot(p, kv_refs[i][keys, HEAD_DIM:], preferred_element_type=F32)
            mixed = part if mixed is None else mixed + part
        a_s[pl.ds(start, BLOCK), :] = a_s[pl.ds(start, BLOCK), :] + mixed

    def per_z(zq, _):
        rows = pl.ds(pl.multiple_of(zq * BLOCK, BLOCK), BLOCK)
        if first:
            m_s[rows, :] = jnp.full((BLOCK, 128), -1e30, F32)
            l_s[rows, :] = jnp.zeros((BLOCK, 128), F32)
            a_s[rows, :] = jnp.zeros((BLOCK, HEAD_DIM), F32)
        else:
            for i in range(3):
                arriving(i, zq).wait()

        def per_key(zk, _):
            accumulate(zq, zk)
            return 0

        lax.fori_loop(0, zq + 1, per_key, 0)
        if last:
            total = jnp.sum(l_s[rows, :], axis=1, keepdims=True)
            o_ref[rows_of(zq - zs[0]), :] = (a_s[rows, :] / total).astype(BF16)
        for i in range(len(kept)):
            leaving(i, zq).start()
        return 0

    lax.fori_loop(*zs, per_z, 0)
    for zq in range(*zs):
        for i in range(len(kept)):
            leaving(i, zq).wait()


def attend(where, q, chunks, state, last, zs=(0, Z)):
    n_pairs = len(chunks) // 2
    first = state is None
    wide = pltpu.HBM((LOCAL, 128), F32)
    vmem = pl.BlockSpec(memory_space=pltpu.VMEM)
    hbm = pl.BlockSpec(memory_space=pltpu.HBM)
    args = [where, q, *chunks]
    if not first:
        args += [pltpu.with_memory_space_constraint(a, pltpu.HBM) for a in state]
    n_vmem = 1 + len(chunks)
    n_rows = (zs[1] - zs[0]) * BLOCK
    pairs = sum(range(1 + zs[0], 1 + zs[1])) * BLOCK * BLOCK * 2 * n_pairs
    return pl.pallas_call(
        functools.partial(attend_body, first, last, n_pairs, zs),
        out_shape=jax.ShapeDtypeStruct((n_rows, HEAD_DIM), BF16) if last else [wide] * 3,
        in_specs=[pl.BlockSpec(memory_space=pltpu.SMEM)]
        + [vmem] * n_vmem
        + [hbm] * (len(args) - 1 - n_vmem),
        out_specs=vmem if last else [hbm] * 3,
        scratch_shapes=[pltpu.VMEM((LOCAL, 128), F32)] * 3
        + [pltpu.SemaphoreType.DMA((3, Z))] * 2,
        compiler_params=params(22),
        cost_estimate=pl.CostEstimate(
            flops=pairs * 4 * HEAD_DIM, transcendentals=pairs, bytes_accessed=n_pairs * 2 * LOCAL * 512
        ),
    )(*args)


def project_body(where_ref, attn_ref, tokens_ref, gain_ref, *refs):
    wo_refs = refs[:8]
    attended_ref, normed_ref, wide_s = refs[8:]
    core, z_own, x_own = where_ref[0], where_ref[1], where_ref[2]
    heads = []
    for c in (core, 1 - core):
        for z in range(Z):
            for e in range(2):
                heads.append(attn_ref[2 * (2 * ((z_own - z) % Z) + c) + e])
    rows = jnp.concatenate(heads, axis=1)
    for i in range(Y):
        y = where_ref[3 + i]
        for x in range(0, X, 2):
            weight = jnp.concatenate(
                [
                    jnp.concatenate([ref[z * X + x], ref[z * X + x + 1]], axis=1)
                    for ref in wo_refs[2 * i : 2 * i + 2]
                    for z in range(Z)
                ],
                axis=0,
            )
            share = jnp.dot(rows, weight, preferred_element_type=F32)
            for side in range(2):
                column = (x_own - x - side) % X * Y + y
                cols = pl.ds(pl.multiple_of(column * 128, 128), 128)
                part = share[:, side * 128 : (side + 1) * 128]
                kept = (tokens_ref[:, cols].astype(F32) + part).astype(BF16)
                attended_ref[:, cols] = kept
                wide_s[:, cols] = kept.astype(F32)
    wide = wide_s[...]
    inverse = lax.rsqrt(jnp.mean(wide * wide, axis=1, keepdims=True) + EPS)
    normed_ref[...] = (wide * inverse * gain_ref[...].astype(F32)).astype(BF16)


def project(where, attn, wo, tokens, gain):
    d = tokens.shape[1]
    vmem = pl.BlockSpec(memory_space=pltpu.VMEM)
    out = jax.ShapeDtypeStruct((ROWS, d), BF16)
    return pl.pallas_call(
        project_body,
        out_shape=[out, out],
        in_specs=[pl.BlockSpec(memory_space=pltpu.SMEM)] + [vmem] * (3 + len(wo)),
        out_specs=[vmem] * 2,
        scratch_shapes=[pltpu.VMEM((ROWS, d), F32)],
        compiler_params=params(14),
        cost_estimate=pl.CostEstimate(
            flops=2 * ROWS * d * d, transcendentals=0, bytes_accessed=2 * d * d
        ),
    )(where, attn, tokens, gain, *wo)


def ffn_body(n_chunks, w_ref, *refs):
    x_refs = refs[:n_chunks]
    o_ref = refs[n_chunks]
    x_s = refs[n_chunks + 1]
    for i in range(n_chunks):
        x_s[i * ROWS : (i + 1) * ROWS, :] = x_refs[i][...]
    tile = 2 * ROWS

    def weight(kind, x):
        return jnp.concatenate(
            [w_ref[z * X + x, kind, c] for z in range(Z) for c in range(C)], axis=1
        )

    def per_tile(t, _):
        rows = x_s[pl.ds(pl.multiple_of(t * tile, tile), tile), :]
        acc = None
        for x in range(X):
            nt = (((1,), (1,)), ((), ()))
            gate = lax.dot_general(rows, weight(0, x), nt, preferred_element_type=F32)
            up = lax.dot_general(rows, weight(1, x), nt, preferred_element_type=F32)
            hidden = (gate / (1.0 + jnp.exp(-gate)) * up).astype(BF16)
            part = jnp.dot(hidden, weight(2, x), preferred_element_type=F32)
            acc = part if acc is None else acc + part
        o_ref[pl.ds(pl.multiple_of(t * tile, tile), tile), :] = acc.astype(BF16)
        return 0

    lax.fori_loop(0, n_chunks * ROWS // tile, per_tile, 0)


def ffn(w, chunks):
    d = chunks[0].shape[1]
    n = len(chunks)
    vmem = pl.BlockSpec(memory_space=pltpu.VMEM)
    return pl.pallas_call(
        functools.partial(ffn_body, n),
        out_shape=jax.ShapeDtypeStruct((n * ROWS, d), BF16),
        in_specs=[vmem] * (n + 1),
        out_specs=vmem,
        scratch_shapes=[pltpu.VMEM((n * ROWS, d), BF16)],
        compiler_params=params(26),
        cost_estimate=pl.CostEstimate(
            flops=6 * n * ROWS * d * X * w.shape[3],
            transcendentals=n * ROWS * X * w.shape[3],
            bytes_accessed=2 * w.size,
        ),
    )(w, *chunks)


def gather_near(own):
    before = along_y(own, 1)
    after = along_y(own, -1)
    return other_core(own), (before, other_core(before)), (after, other_core(after))


def gather_far(before, after):
    half = before.shape[0] // 2
    top = along_y(before[:half], 1)
    bottom = along_y(after[half:], -1)
    far = jnp.concatenate([top, bottom], axis=0)
    return far, other_core(far)


def wide_add(a, b):
    return a.astype(F32) + b.astype(F32)


def shards(
    tokens, queries, keys, values, out_weight, norm_gain, gate_weight, up_weight, down_weight
):
    d = tokens.shape[1]
    core = lax.axis_index("c")
    y = lax.axis_index("y")

    def regroup(array):
        return lax.all_to_all(array, ("z", "x"), split_axis=0, concat_axis=0, tiled=True)

    kv = by_head(keys, values)
    kv = regroup(kv).reshape(LOCAL, 2 * HEAD_DIM)
    kv_c, before, after = gather_near(kv)

    wo = jnp.stack([out_weight] + [along(out_weight, "x", i) for i in range(1, X)])
    wo = lax.optimization_barrier(wo)
    wo = jnp.stack([wo] + [along(wo, "z", i) for i in range(1, Z)])
    wo = wo.reshape(Z * X, *out_weight.shape)

    q = queries.reshape(ROWS, HEADS, HEAD_DIM).transpose(1, 0, 2)
    q = regroup(q).reshape(LOCAL, HEAD_DIM)

    packed = jnp.stack([gate_weight.T, up_weight.T, down_weight])
    packed = packed.reshape(3, 2, packed.shape[1] // 2, packed.shape[2])
    keep = lax.dynamic_index_in_dim(packed, core, 1, keepdims=False)
    send = lax.dynamic_index_in_dim(packed, 1 - core, 1, keepdims=False)
    got = other_core(send)
    both = jnp.stack([jnp.where(core == 0, keep, got), jnp.where(core == 0, got, keep)], axis=1)
    w = lax.all_gather(both.reshape(-1, both.shape[-1]), ("z", "x"), axis=0, tiled=True)
    w = w.reshape(Z * X, *both.shape)

    def where(*steps):
        return jnp.stack([core, y] + [(y + s) % Y for s in steps]).astype(jnp.int32)

    state = attend(where(0), q, [kv, kv_c], None, False)
    far = gather_far(before[0], after[0])
    state = attend(where(-1, 1), q, [*before, *after], state, False)
    low = attend(where(2), q, far, state, True, (0, Z - 1))
    high = attend(where(2), q, far, state, True, (Z - 1, Z))
    attn = jnp.concatenate([low, high], axis=0)

    wo_c, wo_before, wo_after = gather_near(wo)
    wo_far = gather_far(wo_before[0], wo_after[0])
    attn = regroup(attn.reshape(HEADS, ROWS, HEAD_DIM))
    attn, w = lax.optimization_barrier((attn, w))
    attended, normed = project(
        jnp.stack(
            [core, lax.axis_index("z"), lax.axis_index("x")]
            + [(y + s) % Y for s in (0, -1, 1, 2)]
        ).astype(jnp.int32),
        attn,
        [wo, wo_c, *wo_before, *wo_after, *wo_far],
        tokens,
        norm_gain.reshape(1, d),
    )

    normed_c, before, after = gather_near(normed)
    own_part = ffn(w, [normed, normed_c])
    far = gather_far(before[0], after[0])
    near_part = ffn(w, [before[0], after[0], before[1], after[1]])
    far_part = ffn(w, far)

    half = ROWS // 2
    got_own = other_core(own_part[ROWS:])
    got_near = other_core(near_part[2 * ROWS :])
    before = wide_add(near_part[:ROWS], got_near[:ROWS])
    after = wide_add(near_part[ROWS : 2 * ROWS], got_near[ROWS:])
    early_after = along_y(after[half:].astype(BF16), 1)
    early_before = along_y(before[:half].astype(BF16), -1)
    far = wide_add(far_part[:ROWS], other_core(far_part[ROWS:])).astype(BF16)
    far_top = along_y(far[:half], 1)
    far_bottom = along_y(far[half:], -1)
    far_top, far_bottom = lax.optimization_barrier((far_top, far_bottom))
    late_after = along_y(wide_add(after[:half], far_top).astype(BF16), 1)
    late_before = along_y(wide_add(before[half:], far_bottom).astype(BF16), -1)
    own = wide_add(own_part[:ROWS], got_own)
    total = jnp.concatenate(
        [
            own[:half] + wide_add(late_after, early_before),
            own[half:] + wide_add(early_after, late_before),
        ],
        axis=0,
    )
    return attended, (attended.astype(F32) + total).astype(BF16)


def solution(mesh):
    grid = Mesh(mesh.devices.reshape(Z, C, X, Y), ("z", "c", "x", "y"))
    rows = P(("z", "c", "x", "y"), None)
    block = P(("z", "c"), ("x", "y"))
    return jax.shard_map(
        shards,
        mesh=grid,
        in_specs=(rows, rows, rows, rows, block, P(), block, block, P(("x", "y"), ("z", "c"))),
        out_specs=(rows, rows),
        check_vma=False,
    )
```

```python
import functools

import jax
import jax.numpy as jnp
import numpy as np
from jax import lax
from jax.experimental import pallas as pl
from jax.experimental.pallas import tpu as pltpu
from jax.sharding import Mesh
from jax.sharding import PartitionSpec as P


HEAD_DIM = 128
EPS = 1e-05
ROWS = 128
Z, C, X, Y = 4, 2, 4, 4
HEADS = Z * X
BLOCK = X * ROWS
LOCAL = Z * BLOCK
GROUP = 32
SCALE = float(HEAD_DIM**-0.5 * np.log2(np.e))
F32 = jnp.float32
BF16 = jnp.bfloat16


def params(mib):
    return pltpu.CompilerParams(vmem_limit_bytes=mib * 1024 * 1024)


def along(array, axis, step):
    return lax.ppermute(array, axis, [(i, (i + step) % 4) for i in range(4)])


def around(array, way):
    pairs = [(c * Y + i, c * Y + (i + (way if c == 0 else -way)) % Y) for c in range(C) for i in range(Y)]
    return lax.ppermute(array, ("c", "y"), pairs)


def other_core(array):
    return lax.ppermute(array, "c", [(0, 1), (1, 0)])


def by_head_body(keys_ref, values_ref, o_ref):
    n_kv = keys_ref.shape[1] // HEAD_DIM
    for h in range(HEADS):
        g = h * n_kv // HEADS
        cols = slice(g * HEAD_DIM, (g + 1) * HEAD_DIM)
        o_ref[h, :, :HEAD_DIM] = keys_ref[:, cols]
        o_ref[h, :, HEAD_DIM:] = values_ref[:, cols]


def by_head(keys, values):
    vmem = pl.BlockSpec(memory_space=pltpu.VMEM)
    return pl.pallas_call(
        by_head_body,
        out_shape=jax.ShapeDtypeStruct((HEADS, ROWS, 2 * HEAD_DIM), BF16),
        in_specs=[vmem] * 2,
        out_specs=vmem,
        compiler_params=params(8),
    )(keys, values)


def attend_body(first, last, n_pairs, zs, where_ref, q_ref, *refs):
    kv_refs = refs[: 2 * n_pairs]
    refs = refs[2 * n_pairs :]
    given = () if first else refs[:3]
    refs = refs[len(given) :]
    if last:
        o_ref, *refs = refs
        kept = ()
    else:
        kept = refs[:3]
        refs = refs[3:]
    m_s, l_s, a_s, arrived, left = refs
    held = (m_s, l_s, a_s)

    def rows_of(zq):
        return pl.ds(pl.multiple_of(zq * BLOCK, BLOCK), BLOCK)

    def arriving(i, zq):
        rows = rows_of(zq)
        return pltpu.make_async_copy(given[i].at[rows], held[i].at[rows], arrived.at[i, zq])

    def leaving(i, zq):
        rows = rows_of(zq)
        return pltpu.make_async_copy(held[i].at[rows], kept[i].at[rows], left.at[i, zq])

    for zq in range(*zs):
        for i in range(len(given)):
            arriving(i, zq).start()
    c_q = where_ref[0]
    y_q = where_ref[1]
    lanes = BLOCK // 128

    def accumulate(zq, zk):
        start = pl.multiple_of(zq * BLOCK, BLOCK)
        keys = pl.ds(pl.multiple_of(zk * BLOCK, BLOCK), BLOCK)
        q = q_ref[pl.ds(start, BLOCK), :]
        scores = [
            lax.dot_general(
                q, kv_refs[i][keys, :HEAD_DIM], (((1,), (1,)), ((), ())), preferred_element_type=F32
            )
            for i in range(2 * n_pairs)
        ]
        ahead = lax.broadcasted_iota(jnp.int32, (GROUP, 128), 1) - lax.broadcasted_iota(
            jnp.int32, (GROUP, 128), 0
        )
        probs = [[] for _ in range(2 * n_pairs)]
        for low in range(0, BLOCK, GROUP):
            rows = pl.ds(start + low, GROUP)
            tiles = []
            for i in range(2 * n_pairs):
                for lane in range(lanes):
                    tile = scores[i][low : low + GROUP, lane * 128 : (lane + 1) * 128] * SCALE
                    cores = C * (zk - zq) + (0 if i % 2 == 0 else 1 - 2 * c_q)
                    gap = cores * (X * Y * ROWS) + (where_ref[2 + i // 2] - y_q) * ROWS
                    gap = gap + (lane - low // ROWS) * (Y * ROWS) - low % ROWS
                    tiles.append(jnp.where(ahead <= -gap, tile, -1e30))
            m_old = m_s[rows, :]
            peak = jnp.max(functools.reduce(jnp.maximum, tiles), axis=1, keepdims=True)
            m_new = jnp.maximum(m_old, jnp.broadcast_to(peak, m_old.shape))
            alpha = jnp.exp2(m_old - m_new)
            terms = [jnp.exp2(tile - m_new) for tile in tiles]
            m_s[rows, :] = m_new
            l_s[rows, :] = l_s[rows, :] * alpha + functools.reduce(jnp.add, terms)
            a_s[rows, :] = a_s[rows, :] * alpha
            for i in range(2 * n_pairs):
                mine = [t.astype(BF16) for t in terms[i * lanes : (i + 1) * lanes]]
                probs[i].append(jnp.concatenate(mine, axis=1))
        mixed = None
        for i in range(2 * n_pairs):
            p = jnp.concatenate(probs[i], axis=0)
            part = jnp.dot(p, kv_refs[i][keys, HEAD_DIM:], preferred_element_type=F32)
            mixed = part if mixed is None else mixed + part
        a_s[pl.ds(start, BLOCK), :] = a_s[pl.ds(start, BLOCK), :] + mixed

    def per_z(zq, _):
        rows = pl.ds(pl.multiple_of(zq * BLOCK, BLOCK), BLOCK)
        if first:
            m_s[rows, :] = jnp.full((BLOCK, 128), -1e30, F32)
            l_s[rows, :] = jnp.zeros((BLOCK, 128), F32)
            a_s[rows, :] = jnp.zeros((BLOCK, HEAD_DIM), F32)
        else:
            for i in range(3):
                arriving(i, zq).wait()

        def per_key(zk, _):
            accumulate(zq, zk)
            return 0

        lax.fori_loop(0, zq + 1, per_key, 0)
        if last:
            total = jnp.sum(l_s[rows, :], axis=1, keepdims=True)
            o_ref[rows_of(zq - zs[0]), :] = (a_s[rows, :] / total).astype(BF16)
        for i in range(len(kept)):
            leaving(i, zq).start()
        return 0

    lax.fori_loop(*zs, per_z, 0)
    for zq in range(*zs):
        for i in range(len(kept)):
            leaving(i, zq).wait()


def attend(where, q, chunks, state, last, zs=(0, Z)):
    n_pairs = len(chunks) // 2
    first = state is None
    wide = pltpu.HBM((LOCAL, 128), F32)
    vmem = pl.BlockSpec(memory_space=pltpu.VMEM)
    hbm = pl.BlockSpec(memory_space=pltpu.HBM)
    args = [where, q, *chunks]
    if not first:
        args += [pltpu.with_memory_space_constraint(a, pltpu.HBM) for a in state]
    n_vmem = 1 + len(chunks)
    n_rows = (zs[1] - zs[0]) * BLOCK
    pairs = sum(range(1 + zs[0], 1 + zs[1])) * BLOCK * BLOCK * 2 * n_pairs
    return pl.pallas_call(
        functools.partial(attend_body, first, last, n_pairs, zs),
        out_shape=jax.ShapeDtypeStruct((n_rows, HEAD_DIM), BF16) if last else [wide] * 3,
        in_specs=[pl.BlockSpec(memory_space=pltpu.SMEM)]
        + [vmem] * n_vmem
        + [hbm] * (len(args) - 1 - n_vmem),
        out_specs=vmem if last else [hbm] * 3,
        scratch_shapes=[pltpu.VMEM((LOCAL, 128), F32)] * 3
        + [pltpu.SemaphoreType.DMA((3, Z))] * 2,
        compiler_params=params(22),
        cost_estimate=pl.CostEstimate(
            flops=pairs * 4 * HEAD_DIM, transcendentals=pairs, bytes_accessed=n_pairs * 2 * LOCAL * 512
        ),
    )(*args)


def project_body(where_ref, attn_ref, tokens_ref, gain_ref, *refs):
    wo_refs = refs[:8]
    attended_ref, normed_ref, wide_s = refs[8:]
    core, z_own, x_own = where_ref[0], where_ref[1], where_ref[2]
    heads = []
    for c in (core, 1 - core):
        for z in range(Z):
            for e in range(2):
                heads.append(attn_ref[2 * (2 * ((z_own - z) % Z) + c) + e])
    rows = jnp.concatenate(heads, axis=1)
    for i in range(Y):
        y = where_ref[3 + i]
        for x in range(0, X, 2):
            weight = jnp.concatenate(
                [
                    jnp.concatenate([ref[z * X + x], ref[z * X + x + 1]], axis=1)
                    for ref in wo_refs[2 * i : 2 * i + 2]
                    for z in range(Z)
                ],
                axis=0,
            )
            share = jnp.dot(rows, weight, preferred_element_type=F32)
            for side in range(2):
                column = (x_own - x - side) % X * Y + y
                cols = pl.ds(pl.multiple_of(column * 128, 128), 128)
                part = share[:, side * 128 : (side + 1) * 128]
                kept = (tokens_ref[:, cols].astype(F32) + part).astype(BF16)
                attended_ref[:, cols] = kept
                wide_s[:, cols] = kept.astype(F32)
    wide = wide_s[...]
    inverse = lax.rsqrt(jnp.mean(wide * wide, axis=1, keepdims=True) + EPS)
    normed_ref[...] = (wide * inverse * gain_ref[...].astype(F32)).astype(BF16)


def project(where, attn, wo, tokens, gain):
    d = tokens.shape[1]
    vmem = pl.BlockSpec(memory_space=pltpu.VMEM)
    out = jax.ShapeDtypeStruct((ROWS, d), BF16)
    return pl.pallas_call(
        project_body,
        out_shape=[out, out],
        in_specs=[pl.BlockSpec(memory_space=pltpu.SMEM)] + [vmem] * (3 + len(wo)),
        out_specs=[vmem] * 2,
        scratch_shapes=[pltpu.VMEM((ROWS, d), F32)],
        compiler_params=params(14),
        cost_estimate=pl.CostEstimate(
            flops=2 * ROWS * d * d, transcendentals=0, bytes_accessed=2 * d * d
        ),
    )(where, attn, tokens, gain, *wo)


def ffn_body(n_chunks, w_ref, *refs):
    x_refs = refs[:n_chunks]
    o_ref = refs[n_chunks]
    x_s = refs[n_chunks + 1]
    for i in range(n_chunks):
        x_s[i * ROWS : (i + 1) * ROWS, :] = x_refs[i][...]
    tile = 2 * ROWS

    def weight(kind, x):
        return jnp.concatenate(
            [w_ref[z * X + x, kind, c] for z in range(Z) for c in range(C)], axis=1
        )

    def per_tile(t, _):
        rows = x_s[pl.ds(pl.multiple_of(t * tile, tile), tile), :]
        acc = None
        for x in range(X):
            nt = (((1,), (1,)), ((), ()))
            gate = lax.dot_general(rows, weight(0, x), nt, preferred_element_type=F32)
            up = lax.dot_general(rows, weight(1, x), nt, preferred_element_type=F32)
            hidden = (gate / (1.0 + jnp.exp(-gate)) * up).astype(BF16)
            part = jnp.dot(hidden, weight(2, x), preferred_element_type=F32)
            acc = part if acc is None else acc + part
        o_ref[pl.ds(pl.multiple_of(t * tile, tile), tile), :] = acc.astype(BF16)
        return 0

    lax.fori_loop(0, n_chunks * ROWS // tile, per_tile, 0)


def ffn(w, chunks):
    d = chunks[0].shape[1]
    n = len(chunks)
    vmem = pl.BlockSpec(memory_space=pltpu.VMEM)
    return pl.pallas_call(
        functools.partial(ffn_body, n),
        out_shape=jax.ShapeDtypeStruct((n * ROWS, d), BF16),
        in_specs=[vmem] * (n + 1),
        out_specs=vmem,
        scratch_shapes=[pltpu.VMEM((n * ROWS, d), BF16)],
        compiler_params=params(26),
        cost_estimate=pl.CostEstimate(
            flops=6 * n * ROWS * d * X * w.shape[3],
            transcendentals=n * ROWS * X * w.shape[3],
            bytes_accessed=2 * w.size,
        ),
    )(w, *chunks)


def gather_near(own):
    before = around(own, 1)
    after = around(own, -1)
    return other_core(own), (before, other_core(after)), (after, other_core(before))


def gather_far(before):
    far = around(before, 1)
    return far, other_core(far)


def wide_add(a, b):
    return a.astype(F32) + b.astype(F32)


def shards(
    tokens, queries, keys, values, out_weight, norm_gain, gate_weight, up_weight, down_weight
):
    d = tokens.shape[1]
    core = lax.axis_index("c")
    y = lax.axis_index("y")

    def regroup(array):
        return lax.all_to_all(array, ("z", "x"), split_axis=0, concat_axis=0, tiled=True)

    kv = by_head(keys, values)
    kv = regroup(kv).reshape(LOCAL, 2 * HEAD_DIM)
    kv_c, before, after = gather_near(kv)

    wo = jnp.stack([out_weight] + [along(out_weight, "x", i) for i in range(1, X)])
    wo = lax.optimization_barrier(wo)
    wo = jnp.stack([wo] + [along(wo, "z", i) for i in range(1, Z)])
    wo = wo.reshape(Z * X, *out_weight.shape)

    q = queries.reshape(ROWS, HEADS, HEAD_DIM).transpose(1, 0, 2)
    q = regroup(q).reshape(LOCAL, HEAD_DIM)

    packed = jnp.stack([gate_weight.T, up_weight.T, down_weight])
    packed = packed.reshape(3, 2, packed.shape[1] // 2, packed.shape[2])
    keep = lax.dynamic_index_in_dim(packed, core, 1, keepdims=False)
    send = lax.dynamic_index_in_dim(packed, 1 - core, 1, keepdims=False)
    got = other_core(send)
    both = jnp.stack([jnp.where(core == 0, keep, got), jnp.where(core == 0, got, keep)], axis=1)
    w = lax.all_gather(both.reshape(-1, both.shape[-1]), ("z", "x"), axis=0, tiled=True)
    w = w.reshape(Z * X, *both.shape)

    side = 2 * core - 1

    def where(*steps):
        return jnp.stack([core, y] + [(y + s) % Y for s in steps]).astype(jnp.int32)

    state = attend(where(0), q, [kv, kv_c], None, False)
    far = gather_far(before[0])
    state = attend(where(side, -side), q, [*before, *after], state, False)
    low = attend(where(2), q, far, state, True, (0, Z - 1))
    high = attend(where(2), q, far, state, True, (Z - 1, Z))
    attn = jnp.concatenate([low, high], axis=0)

    wo_c, wo_before, wo_after = gather_near(wo)
    wo_far = gather_far(wo_before[0])
    attn = regroup(attn.reshape(HEADS, ROWS, HEAD_DIM))
    attn, w = lax.optimization_barrier((attn, w))
    attended, normed = project(
        jnp.stack(
            [core, lax.axis_index("z"), lax.axis_index("x")]
            + [(y + s) % Y for s in (0, side, -side, 2)]
        ).astype(jnp.int32),
        attn,
        [wo, wo_c, *wo_before, *wo_after, *wo_far],
        tokens,
        norm_gain.reshape(1, d),
    )

    normed_c, before, after = gather_near(normed)
    own_part = ffn(w, [normed, normed_c])
    far = gather_far(before[0])
    near_part = ffn(w, [before[0], after[0], before[1], after[1]])
    far_part = ffn(w, far)

    got_own = other_core(own_part[ROWS:])
    got_near = other_core(near_part[2 * ROWS :])
    before = wide_add(near_part[:ROWS], got_near[ROWS:])
    after = wide_add(near_part[ROWS : 2 * ROWS], got_near[:ROWS])
    far = wide_add(far_part[:ROWS], other_core(far_part[ROWS:])).astype(BF16)
    far = around(far, 1)
    before, after = lax.optimization_barrier((before.astype(BF16), after))
    before = around(before, -1)
    after = around(wide_add(after, far).astype(BF16), 1)
    own = wide_add(own_part[:ROWS], got_own)
    total = own + wide_add(before, after)
    return attended, (attended.astype(F32) + total).astype(BF16)


def solution(mesh):
    grid = Mesh(mesh.devices.reshape(Z, C, X, Y), ("z", "c", "x", "y"))
    rows = P(("z", "c", "x", "y"), None)
    block = P(("z", "c"), ("x", "y"))
    return jax.shard_map(
        shards,
        mesh=grid,
        in_specs=(rows, rows, rows, rows, block, P(), block, block, P(("x", "y"), ("z", "c"))),
        out_specs=(rows, rows),
        check_vma=False,
    )
```

```python
import functools

import jax
import jax.numpy as jnp
import numpy as np
from jax import lax
from jax.experimental import pallas as pl
from jax.experimental.pallas import tpu as pltpu
from jax.sharding import Mesh
from jax.sharding import PartitionSpec as P


HEAD_DIM = 128
EPS = 1e-05
ROWS = 128
Z, C, X, Y = 4, 2, 4, 4
HEADS = Z * X
BLOCK = X * ROWS
LOCAL = Z * BLOCK
GROUP = 32
SCALE = float(HEAD_DIM**-0.5 * np.log2(np.e))
F32 = jnp.float32
BF16 = jnp.bfloat16


def params(mib):
    return pltpu.CompilerParams(vmem_limit_bytes=mib * 1024 * 1024)


def along(array, axis, step):
    return lax.ppermute(array, axis, [(i, (i + step) % 4) for i in range(4)])


def around(array, way):
    pairs = [(c * Y + i, c * Y + (i + (way if c == 0 else -way)) % Y) for c in range(C) for i in range(Y)]
    return lax.ppermute(array, ("c", "y"), pairs)


def other_core(array):
    return lax.ppermute(array, "c", [(0, 1), (1, 0)])


def by_head_body(keys_ref, values_ref, o_ref):
    n_kv = keys_ref.shape[1] // HEAD_DIM
    for h in range(HEADS):
        g = h * n_kv // HEADS
        cols = slice(g * HEAD_DIM, (g + 1) * HEAD_DIM)
        o_ref[h, :, :HEAD_DIM] = keys_ref[:, cols]
        o_ref[h, :, HEAD_DIM:] = values_ref[:, cols]


def by_head(keys, values):
    vmem = pl.BlockSpec(memory_space=pltpu.VMEM)
    return pl.pallas_call(
        by_head_body,
        out_shape=jax.ShapeDtypeStruct((HEADS, ROWS, 2 * HEAD_DIM), BF16),
        in_specs=[vmem] * 2,
        out_specs=vmem,
        compiler_params=params(8),
    )(keys, values)


def attend_body(first, last, n_pairs, zs, where_ref, q_ref, *refs):
    kv_refs = refs[: 2 * n_pairs]
    refs = refs[2 * n_pairs :]
    given = () if first else refs[:3]
    refs = refs[len(given) :]
    if last:
        o_ref, *refs = refs
        kept = ()
    else:
        kept = refs[:3]
        refs = refs[3:]
    m_s, l_s, a_s, arrived, left = refs
    held = (m_s, l_s, a_s)

    def rows_of(zq):
        return pl.ds(pl.multiple_of(zq * BLOCK, BLOCK), BLOCK)

    def arriving(i, zq):
        rows = rows_of(zq)
        return pltpu.make_async_copy(given[i].at[rows], held[i].at[rows], arrived.at[i, zq])

    def leaving(i, zq):
        rows = rows_of(zq)
        return pltpu.make_async_copy(held[i].at[rows], kept[i].at[rows], left.at[i, zq])

    for zq in range(*zs):
        for i in range(len(given)):
            arriving(i, zq).start()
    c_q = where_ref[0]
    y_q = where_ref[1]
    lanes = BLOCK // 128

    def accumulate(zq, zk):
        start = pl.multiple_of(zq * BLOCK, BLOCK)
        keys = pl.ds(pl.multiple_of(zk * BLOCK, BLOCK), BLOCK)
        q = q_ref[pl.ds(start, BLOCK), :]
        scores = [
            lax.dot_general(
                q, kv_refs[i][keys, :HEAD_DIM], (((1,), (1,)), ((), ())), preferred_element_type=F32
            )
            for i in range(2 * n_pairs)
        ]
        ahead = lax.broadcasted_iota(jnp.int32, (GROUP, 128), 1) - lax.broadcasted_iota(
            jnp.int32, (GROUP, 128), 0
        )
        probs = [[] for _ in range(2 * n_pairs)]
        for low in range(0, BLOCK, GROUP):
            rows = pl.ds(start + low, GROUP)
            tiles = []
            for i in range(2 * n_pairs):
                for lane in range(lanes):
                    tile = scores[i][low : low + GROUP, lane * 128 : (lane + 1) * 128] * SCALE
                    cores = C * (zk - zq) + (0 if i % 2 == 0 else 1 - 2 * c_q)
                    gap = cores * (X * Y * ROWS) + (where_ref[2 + i // 2] - y_q) * ROWS
                    gap = gap + (lane - low // ROWS) * (Y * ROWS) - low % ROWS
                    tiles.append(jnp.where(ahead <= -gap, tile, -1e30))
            m_old = m_s[rows, :]
            peak = jnp.max(functools.reduce(jnp.maximum, tiles), axis=1, keepdims=True)
            m_new = jnp.maximum(m_old, jnp.broadcast_to(peak, m_old.shape))
            alpha = jnp.exp2(m_old - m_new)
            terms = [jnp.exp2(tile - m_new) for tile in tiles]
            m_s[rows, :] = m_new
            l_s[rows, :] = l_s[rows, :] * alpha + functools.reduce(jnp.add, terms)
            a_s[rows, :] = a_s[rows, :] * alpha
            for i in range(2 * n_pairs):
                mine = [t.astype(BF16) for t in terms[i * lanes : (i + 1) * lanes]]
                probs[i].append(jnp.concatenate(mine, axis=1))
        mixed = None
        for i in range(2 * n_pairs):
            p = jnp.concatenate(probs[i], axis=0)
            part = jnp.dot(p, kv_refs[i][keys, HEAD_DIM:], preferred_element_type=F32)
            mixed = part if mixed is None else mixed + part
        a_s[pl.ds(start, BLOCK), :] = a_s[pl.ds(start, BLOCK), :] + mixed

    def per_z(zq, _):
        rows = pl.ds(pl.multiple_of(zq * BLOCK, BLOCK), BLOCK)
        if first:
            m_s[rows, :] = jnp.full((BLOCK, 128), -1e30, F32)
            l_s[rows, :] = jnp.zeros((BLOCK, 128), F32)
            a_s[rows, :] = jnp.zeros((BLOCK, HEAD_DIM), F32)
        else:
            for i in range(3):
                arriving(i, zq).wait()

        def per_key(zk, _):
            accumulate(zq, zk)
            return 0

        lax.fori_loop(0, zq + 1, per_key, 0)
        if last:
            total = jnp.sum(l_s[rows, :], axis=1, keepdims=True)
            o_ref[rows_of(zq - zs[0]), :] = (a_s[rows, :] / total).astype(BF16)
        for i in range(len(kept)):
            leaving(i, zq).start()
        return 0

    lax.fori_loop(*zs, per_z, 0)
    for zq in range(*zs):
        for i in range(len(kept)):
            leaving(i, zq).wait()


def attend(where, q, chunks, state, last, zs=(0, Z)):
    n_pairs = len(chunks) // 2
    first = state is None
    wide = pltpu.HBM((LOCAL, 128), F32)
    vmem = pl.BlockSpec(memory_space=pltpu.VMEM)
    hbm = pl.BlockSpec(memory_space=pltpu.HBM)
    args = [where, q, *chunks]
    if not first:
        args += [pltpu.with_memory_space_constraint(a, pltpu.HBM) for a in state]
    n_vmem = 1 + len(chunks)
    n_rows = (zs[1] - zs[0]) * BLOCK
    pairs = sum(range(1 + zs[0], 1 + zs[1])) * BLOCK * BLOCK * 2 * n_pairs
    return pl.pallas_call(
        functools.partial(attend_body, first, last, n_pairs, zs),
        out_shape=jax.ShapeDtypeStruct((n_rows, HEAD_DIM), BF16) if last else [wide] * 3,
        in_specs=[pl.BlockSpec(memory_space=pltpu.SMEM)]
        + [vmem] * n_vmem
        + [hbm] * (len(args) - 1 - n_vmem),
        out_specs=vmem if last else [hbm] * 3,
        scratch_shapes=[pltpu.VMEM((LOCAL, 128), F32)] * 3
        + [pltpu.SemaphoreType.DMA((3, Z))] * 2,
        compiler_params=params(22),
        cost_estimate=pl.CostEstimate(
            flops=pairs * 4 * HEAD_DIM, transcendentals=pairs, bytes_accessed=n_pairs * 2 * LOCAL * 512
        ),
    )(*args)


def project_body(where_ref, attn_ref, tokens_ref, gain_ref, *refs):
    wo_refs = refs[:8]
    attended_ref, normed_ref, wide_s = refs[8:]
    core, z_own, x_own = where_ref[0], where_ref[1], where_ref[2]
    heads = []
    for c in (core, 1 - core):
        for z in range(Z):
            for e in range(2):
                heads.append(attn_ref[2 * (2 * ((z_own - z) % Z) + c) + e])
    rows = jnp.concatenate(heads, axis=1)
    for i in range(Y):
        y = where_ref[3 + i]
        for x in range(0, X, 2):
            weight = jnp.concatenate(
                [
                    jnp.concatenate([ref[z * X + x], ref[z * X + x + 1]], axis=1)
                    for ref in wo_refs[2 * i : 2 * i + 2]
                    for z in range(Z)
                ],
                axis=0,
            )
            share = jnp.dot(rows, weight, preferred_element_type=F32)
            for side in range(2):
                column = (x_own - x - side) % X * Y + y
                cols = pl.ds(pl.multiple_of(column * 128, 128), 128)
                part = share[:, side * 128 : (side + 1) * 128]
                kept = (tokens_ref[:, cols].astype(F32) + part).astype(BF16)
                attended_ref[:, cols] = kept
                wide_s[:, cols] = kept.astype(F32)
    wide = wide_s[...]
    inverse = lax.rsqrt(jnp.mean(wide * wide, axis=1, keepdims=True) + EPS)
    normed_ref[...] = (wide * inverse * gain_ref[...].astype(F32)).astype(BF16)


def project(where, attn, wo, tokens, gain):
    d = tokens.shape[1]
    vmem = pl.BlockSpec(memory_space=pltpu.VMEM)
    out = jax.ShapeDtypeStruct((ROWS, d), BF16)
    return pl.pallas_call(
        project_body,
        out_shape=[out, out],
        in_specs=[pl.BlockSpec(memory_space=pltpu.SMEM)] + [vmem] * (3 + len(wo)),
        out_specs=[vmem] * 2,
        scratch_shapes=[pltpu.VMEM((ROWS, d), F32)],
        compiler_params=params(14),
        cost_estimate=pl.CostEstimate(
            flops=2 * ROWS * d * d, transcendentals=0, bytes_accessed=2 * d * d
        ),
    )(where, attn, tokens, gain, *wo)


def ffn_body(n_chunks, w_ref, *refs):
    x_refs = refs[:n_chunks]
    o_ref = refs[n_chunks]
    x_s = refs[n_chunks + 1]
    for i in range(n_chunks):
        x_s[i * ROWS : (i + 1) * ROWS, :] = x_refs[i][...]
    tile = 2 * ROWS

    def weight(kind, x):
        return jnp.concatenate(
            [w_ref[z * X + x, kind, c] for z in range(Z) for c in range(C)], axis=1
        )

    def per_tile(t, _):
        rows = x_s[pl.ds(pl.multiple_of(t * tile, tile), tile), :]
        acc = None
        for x in range(X):
            nt = (((1,), (1,)), ((), ()))
            gate = lax.dot_general(rows, weight(0, x), nt, preferred_element_type=F32)
            up = lax.dot_general(rows, weight(1, x), nt, preferred_element_type=F32)
            hidden = (gate / (1.0 + jnp.exp(-gate)) * up).astype(BF16)
            part = jnp.dot(hidden, weight(2, x), preferred_element_type=F32)
            acc = part if acc is None else acc + part
        o_ref[pl.ds(pl.multiple_of(t * tile, tile), tile), :] = acc.astype(BF16)
        return 0

    lax.fori_loop(0, n_chunks * ROWS // tile, per_tile, 0)


def ffn(w, chunks):
    d = chunks[0].shape[1]
    n = len(chunks)
    vmem = pl.BlockSpec(memory_space=pltpu.VMEM)
    return pl.pallas_call(
        functools.partial(ffn_body, n),
        out_shape=jax.ShapeDtypeStruct((n * ROWS, d), BF16),
        in_specs=[vmem] * (n + 1),
        out_specs=vmem,
        scratch_shapes=[pltpu.VMEM((n * ROWS, d), BF16)],
        compiler_params=params(26),
        cost_estimate=pl.CostEstimate(
            flops=6 * n * ROWS * d * X * w.shape[3],
            transcendentals=n * ROWS * X * w.shape[3],
            bytes_accessed=2 * w.size,
        ),
    )(w, *chunks)


def gather_near(own):
    before = around(own, 1)
    after = around(own, -1)
    return other_core(own), (before, other_core(after)), (after, other_core(before))


def gather_far(before):
    far = around(before, 1)
    return far, other_core(far)


def wide_add(a, b):
    return a.astype(F32) + b.astype(F32)


def shards(
    tokens, queries, keys, values, out_weight, norm_gain, gate_weight, up_weight, down_weight
):
    d = tokens.shape[1]
    core = lax.axis_index("c")
    y = lax.axis_index("y")

    def regroup(array):
        return lax.all_to_all(array, ("z", "x"), split_axis=0, concat_axis=0, tiled=True)

    kv = by_head(keys, values)
    kv = regroup(kv).reshape(LOCAL, 2 * HEAD_DIM)
    kv_c, before, after = gather_near(kv)

    wo = jnp.stack([out_weight] + [along(out_weight, "x", i) for i in range(1, X)])
    wo = lax.optimization_barrier(wo)
    wo = jnp.stack([wo] + [along(wo, "z", i) for i in range(1, Z)])
    wo = wo.reshape(Z * X, *out_weight.shape)

    q = queries.reshape(ROWS, HEADS, HEAD_DIM).transpose(1, 0, 2)
    q = regroup(q).reshape(LOCAL, HEAD_DIM)

    packed = jnp.stack([gate_weight.T, up_weight.T, down_weight])
    packed = packed.reshape(3, 2, packed.shape[1] // 2, packed.shape[2])
    keep = lax.dynamic_index_in_dim(packed, core, 1, keepdims=False)
    send = lax.dynamic_index_in_dim(packed, 1 - core, 1, keepdims=False)
    got = other_core(send)
    both = jnp.stack([jnp.where(core == 0, keep, got), jnp.where(core == 0, got, keep)], axis=1)
    w = lax.all_gather(both.reshape(-1, both.shape[-1]), ("z", "x"), axis=0, tiled=True)
    w = w.reshape(Z * X, *both.shape)

    side = 2 * core - 1

    def where(*steps):
        return jnp.stack([core, y] + [(y + s) % Y for s in steps]).astype(jnp.int32)

    state = attend(where(0), q, [kv, kv_c], None, False)
    far = gather_far(before[0])
    state = attend(where(side, -side), q, [*before, *after], state, False)
    low = attend(where(2), q, far, state, True, (0, Z - 1))
    high = attend(where(2), q, far, state, True, (Z - 1, Z))
    attn = jnp.concatenate([low, high], axis=0)

    wo_c, wo_before, wo_after = gather_near(wo)
    wo_far = gather_far(wo_before[0])
    attn = regroup(attn.reshape(HEADS, ROWS, HEAD_DIM))
    attn, w = lax.optimization_barrier((attn, w))
    attended, normed = project(
        jnp.stack(
            [core, lax.axis_index("z"), lax.axis_index("x")]
            + [(y + s) % Y for s in (0, side, -side, 2)]
        ).astype(jnp.int32),
        attn,
        [wo, wo_c, *wo_before, *wo_after, *wo_far],
        tokens,
        norm_gain.reshape(1, d),
    )

    normed_c, before, after = gather_near(normed)
    own_part = ffn(w, [normed, normed_c])
    far = gather_far(before[0])
    near_part = ffn(w, [before[0], after[0], before[1], after[1]])
    far_part = ffn(w, far)

    got_own = other_core(own_part[ROWS:])
    got_near = other_core(near_part[2 * ROWS :])
    before = wide_add(near_part[:ROWS], got_near[ROWS:])
    after = wide_add(near_part[ROWS : 2 * ROWS], got_near[:ROWS])
    far = wide_add(far_part[:ROWS], other_core(far_part[ROWS:])).astype(BF16)
    half = ROWS // 2
    far_top = around(far[:half], 1)
    far_bottom = around(far[half:], -1)
    early_after = around(after[half:].astype(BF16), 1)
    early_before = around(before[:half].astype(BF16), -1)
    far_top, far_bottom = lax.optimization_barrier((far_top, far_bottom))
    late_after = around(wide_add(after[:half], far_top).astype(BF16), 1)
    late_before = around(wide_add(before[half:], far_bottom).astype(BF16), -1)
    own = wide_add(own_part[:ROWS], got_own)
    total = jnp.concatenate(
        [
            own[:half] + wide_add(late_after, early_before),
            own[half:] + wide_add(early_after, late_before),
        ],
        axis=0,
    )
    return attended, (attended.astype(F32) + total).astype(BF16)


def solution(mesh):
    grid = Mesh(mesh.devices.reshape(Z, C, X, Y), ("z", "c", "x", "y"))
    rows = P(("z", "c", "x", "y"), None)
    block = P(("z", "c"), ("x", "y"))
    return jax.shard_map(
        shards,
        mesh=grid,
        in_specs=(rows, rows, rows, rows, block, P(), block, block, P(("x", "y"), ("z", "c"))),
        out_specs=(rows, rows),
        check_vma=False,
    )
```
